32 devices in a mesh: row: 4 (over x, core), col: 8 (over z, y).
Axes of the slice: x: 2, y: 2, z: 4, core: 2. Of those that a mesh axis runs over, the one named last changes fastest.
Arguments:
- hamiltonian: bfloat16 [2912, 2912], P('row', 'col'), may hold values from -6 to 6
- new_atom: int32 [224], replicated, may hold values from 0 to 223, as said below
- pattern: int32 [224, 224], P('row', 'col'), may hold values 0 or 1
Outputs:
- sign_matrix: float32 [2912, 2912], P('row', 'col')
The draws below stay inside these ranges and needn't reach their ends.
Inputs may be any that keep to these rules, and one draw needn't show every extreme that they name: `new_atom`: each old atom appears once. Block column b holds atoms b * 28 to (b + 1) * 28 - 1 in both orders. For each new block column d and each v from 0 to 27, exactly one atom of new block column d comes from old block column (d - 1 - (v mod 8)) mod 8, so the number of atoms that old block column b sends to new block column (b + k) mod 8 is the number of such v with (1 + v) mod 8 = k.
All inputs are finite; a program needn't handle non-finite values. No bound on the sum of `pattern` on one device may be relied on, other than what follows from the above.
Results may differ from the reference program's by a relative error of at most 0.0029.
Values may be sent and summed in bfloat16 or wider, within the bound.
A program may use at most 64 MiB of HBM per device.

```python
import jax
import jax.numpy as jnp
from jax import lax

NBF = 13
ATOM_COL = 28
ATOMS = 224
ORDER = 2912
N_COL = 8


def draw_new_atom(key, part):
    slot_key, arrive_key = jax.random.split(jax.random.fold_in(key, 17))
    slot_keys = jax.random.split(slot_key, N_COL)
    arrive_keys = jax.random.split(arrive_key, N_COL)
    slot_inverse = jax.vmap(lambda k: jax.random.permutation(k, ATOM_COL))(slot_keys).astype(jnp.int32)
    arrival = jax.vmap(lambda k: jax.random.permutation(k, ATOM_COL))(arrive_keys).astype(jnp.int32)
    target = jnp.arange(N_COL, dtype=jnp.int32)[:, None]
    source = (target - 1 - arrival % N_COL) % N_COL
    old_atom = source * ATOM_COL + slot_inverse[source, arrival]
    return old_atom.reshape(-1).astype(jnp.int32)


def set_ends(result, key, smallest, top_value):
    dims = result.shape
    spot = [jax.random.randint(jax.random.fold_in(key, axis), (), 0, dims[axis]) for axis in range(len(dims))]
    result = result.at[tuple(spot)].set(smallest)
    longest = dims.index(max(dims))
    spot[longest] = (spot[longest] + 1) % dims[longest]
    return result.at[tuple(spot)].set(top_value)


def block_scale(key, dims, cuts, smallest, largest):
    gain, own = 1.0, jax.random.fold_in(key, 6)
    for dim, blocks in cuts:
        heights = jnp.exp(jax.random.uniform(jax.random.fold_in(own, dim), (blocks,), jnp.float32, smallest / len(cuts), largest / len(cuts)))
        gain = gain * jnp.repeat(heights, dims[dim] // blocks).reshape([-1 if axis == dim else 1 for axis in range(len(dims))])
    return gain


def normal_values(stream_key, dims, deviation, most, shards=(), held_as=jnp.bfloat16):
    result = jax.random.normal(stream_key, dims, jnp.float32) * deviation
    if len(shards) > 0:
        result = block_scale(stream_key, dims, shards, -0.22, 0.18) * result
    return jnp.clip(result, min=-most, max=most).astype(held_as)


def setup_inputs(seed: int = 0) -> dict:
    streams_of = jax.random.split(jax.random.key(seed), 4)
    hamiltonian = normal_values(streams_of[0], (ORDER, ORDER), 1.0, 6.0, ((0, 4), (1, 8)))
    new_atom = draw_new_atom(jax.random.fold_in(streams_of[3], 71), 0)
    pattern = set_ends((jax.random.randint(streams_of[2], (ATOMS, ATOMS), 0, 3) < 1).astype(jnp.int32), jax.random.fold_in(streams_of[2], 1), 0, 1)
    return dict(hamiltonian=hamiltonian, new_atom=new_atom, pattern=pattern)


def reference(hamiltonian, new_atom, pattern):
    order_all = ATOMS * NBF
    index = (new_atom[:, None] * NBF + jnp.arange(NBF, dtype=jnp.int32)[None, :]).reshape(-1).astype(jnp.int32)
    moved = jnp.take(jnp.take(hamiltonian, index, axis=0), index, axis=1)
    keep = jnp.broadcast_to(pattern.astype(jnp.float32)[:, None, :, None], (ATOMS, NBF, ATOMS, NBF)).reshape(order_all, order_all)
    masked = moved.astype(jnp.float32) * keep
    total = jnp.sum(masked * masked)
    start = (masked * lax.rsqrt(total / order_all)).astype(jnp.bfloat16)
    square = (jnp.dot(start, start, preferred_element_type=jnp.float32) * keep).astype(jnp.bfloat16)
    cube = jnp.dot(start, square, preferred_element_type=jnp.float32) * keep
    return keep * (1.5 * start.astype(jnp.float32) - 0.5 * cube)
```

```python
import functools

import jax
import jax.numpy as jnp
import numpy as np
from jax import lax
from jax.experimental import pallas as pl
from jax.experimental.pallas import tpu as pltpu
from jax.sharding import PartitionSpec as P

NBF = 13
LANE = 128
BF = jnp.bfloat16
F32 = jnp.float32
I32 = jnp.int32
MESH = pl.DeviceIdType.MESH
FAR = -1.0e6


def up(n, k):
    return -(-n // k) * k


def mm(a, b):
    return jnp.dot(a, b, preferred_element_type=F32)


def mm_nt(a, b):
    return lax.dot_general(a, b, (((1,), (1,)), ((), ())), preferred_element_type=F32)


def iota(shape, axis):
    return lax.broadcasted_iota(I32, shape, axis)


def fiota(shape, axis):
    return iota(shape, axis).astype(F32)


def whole_part(x, n):
    return jnp.floor((x + 0.5) * (1.0 / n))


def expand(sel, lo, start, size):
    u = fiota((lo.shape[0], size), 1) - lo
    hit = sel & (u >= 0.0) & (u < NBF)
    return jnp.sum(jnp.where(hit, u + (start + 1.0), 0.0), axis=0, keepdims=True) - 1.0


def onehot(rows, places, offset=0):
    i = fiota((rows, places.shape[1]), 0) + float(offset)
    return jnp.where(i == places, 1.0, 0.0).astype(BF)


class Plan:
    def __init__(self, n_row, n_col, rows, cols, ar, ac):
        self.n_row, self.n_col, self.rows, self.cols, self.ar, self.ac = n_row, n_col, rows, cols, ar, ac
        self.ratio = n_col // n_row
        self.nx = n_row // 2
        self.outer = n_col // 2
        self.av = up(ac, 16)
        self.w = n_col * self.av
        self.blk = up(cols, LANE)
        self.live = up(rows, 16)
        self.wide = up(rows, LANE)
        count = np.bincount((1 + np.arange(ac)) % n_col, minlength=n_col)
        self.slot = up(int(count.max()) * NBF, 16)
        r = self.ratio
        pair = [
            sum(int(count[(r * k + g - b) % n_col]) for b in range(r) for g in range(r)) for k in range(n_row)
        ]
        self.sl = up(max(pair) * NBF, 16)
        self.slp = up(self.sl, LANE)
        own = pair[0] * NBF // 16 * 16
        chip = (pair[0] + min(pair[1], pair[n_row - 1])) * NBF // 16 * 16
        rest = self.live - chip
        last = up(rest // 4, 16)
        ends = [0, own, chip, self.live - last, self.live]
        self.starts, self.sizes = ends[:-1], [b - a for a, b in zip(ends, ends[1:])]
        self.joff = [(0, self.blk - LANE), (self.blk - LANE, LANE)]


def kernel(
    s_, order, h_ref, na_ref, pat_ref, out_ref,
    hv, hp, xs, rin, pp, pt_all, mr, kq, panel, left, racc, rt, rx, xm, fm, sta, stb, cac, tot, tot_all,
    h_sem, x_send, x_recv, p_send, p_recv, t_send, t_recv, g_send, g_recv, r_send, r_recv, f_send,
):
    n_row, n_col, ratio, nx, outer = s_.n_row, s_.n_col, s_.ratio, s_.nx, s_.outer
    ac, ar, av, W, blk, live, wide = s_.ac, s_.ar, s_.av, s_.w, s_.blk, s_.live, s_.wide
    slot, sl, slp = s_.slot, s_.sl, s_.slp
    row = lax.axis_index("row")
    col = lax.axis_index("col")
    hi, lo = col // 2, col % 2
    x, core = row // 2, row % 2
    peer = x * 2 + 1 - core
    n_piece = len(s_.sizes)
    slots = n_col * slot

    h_copy = pltpu.make_async_copy(h_ref, hv, h_sem.at[0])
    h_copy.start()
    barrier = pltpu.get_barrier_semaphore()
    for k in range(1, n_row):
        pl.semaphore_signal(barrier, inc=1, device_id={"row": (row + k) % n_row, "col": col}, device_id_type=MESH)
    for k in range(1, n_col):
        pl.semaphore_signal(barrier, inc=1, device_id={"row": row, "col": (col + k) % n_col}, device_id_type=MESH)

    rowf, colf, xf, coref, peerf = [i.astype(F32) for i in (row, col, x, core, peer)]

    def places(w):
        d = whole_part(w, av)
        v = w - d * av
        return d, v, v < ac

    def source(na, d):
        b = whole_part(na, ac)
        src = whole_part(b, ratio)
        home = whole_part(d, ratio)
        far = jnp.where(whole_part(src, 2) == whole_part(home, 2), 1.0, 2.0)
        return b, src, home, jnp.where(src == home, 0.0, far)

    wc, wr = fiota((W, 1), 0), fiota((1, W), 1)
    dc, vc, okc = places(wc)
    dr, vr, okr = places(wr)
    atoms = na_ref[...].astype(F32)
    here = (fiota((W, atoms.shape[1]), 1) == dc * ac + vc) & okc
    nac = jnp.sum(jnp.where(here, atoms, 0.0), axis=1, keepdims=True)
    nar = jnp.sum(jnp.where(fiota((W, W), 0) == wr, nac, 0.0), axis=0, keepdims=True)
    bc, srcc, homec, grpc = source(nac, dc)
    br, srcr, homer, grpr = source(nar, dr)
    before = wr < wc

    def rank(hit):
        return jnp.sum(jnp.where(hit & okr, 1.0, 0.0), axis=1, keepdims=True)

    rank_slot = rank((dr == dc) & (br == bc) & before)
    rank_pair = rank((homer == homec) & (srcr == srcc) & before)
    rank_all = rank((homer == homec) & ((grpr < grpc) | ((grpr == grpc) & before)))
    old_at = NBF * (nac - srcc * ar)
    kx = whole_part(homec, 2) - xf
    kx = jnp.where(kx < 0.0, kx + nx, kx)
    kc = homec - 2.0 * whole_part(homec, 2)
    kc = jnp.where(kc == coref, 0.0, 1.0)
    from_me = okc & (srcc == rowf)
    to_me = okc & (homec == rowf)
    out_place = expand(from_me, old_at, (2.0 * kx + kc) * slp + NBF * rank_pair, wide)
    own_place = expand(from_me & to_me, old_at, NBF * rank_all, wide)

    def other(sign, k):
        return ((x + sign * (k // 2) + nx) % nx) * 2 + (core + k % 2) % 2

    in_place = {
        k: expand(to_me & (srcc == other(-1, k).astype(F32)), NBF * rank_pair, NBF * rank_all, slp)
        for k in range(1, n_row)
    }

    pp[...] = jnp.zeros_like(pp)
    pp[0:ar, 0:ac] = pat_ref[...].astype(F32).astype(BF)
    flip = jnp.where(iota((av, LANE), 0) == iota((av, LANE), 1), 1.0, 0.0).astype(BF)
    pt_all[col] = mm_nt(flip, pp[...]).astype(BF)
    hp[...] = jnp.zeros_like(hp)
    rin[:, sl:, :] = jnp.zeros((n_row - 1, slp - sl, blk), BF)
    rt[:, live:, :] = jnp.zeros((n_row, wide - live, blk), BF)
    sta[:, live:, :] = jnp.zeros((n_row, wide - live, sta.shape[2]), BF)
    stb[:, live:, :] = jnp.zeros((n_row, wide - live, stb.shape[2]), BF)
    tot[...] = jnp.zeros_like(tot)
    racc[...] = jnp.zeros_like(racc)
    h_copy.wait()
    hp[0 : s_.rows, 0 : s_.cols] = hv[...]

    def pick(k):
        xs[k - 1] = mm(onehot(sl, out_place, k * slp), hp[...]).astype(BF)

    def piece(c, p):
        return panel.at[c, pl.ds(s_.starts[p], s_.sizes[p]), :]

    def assemble(p):
        i0, n = s_.starts[p], s_.sizes[p]
        part = None
        if p < 2:
            part = mm(onehot(n, own_place, i0), hp[...])
        for k in range(1, n_row):
            if p >= (1 if k == 1 else 2):
                more = mm(onehot(n, in_place[k], i0), rin[k - 1])
                part = more if part is None else part + more
        panel[col, i0 : i0 + n, :] = part.astype(BF)

    pl.semaphore_wait(barrier, n_row + n_col - 2)

    def x_copy(k):
        return pltpu.make_async_remote_copy(
            src_ref=xs.at[k - 1], dst_ref=rin.at[k - 1, pl.ds(0, sl), :],
            send_sem=x_send.at[k], recv_sem=x_recv.at[k],
            device_id={"row": other(1, k), "col": col}, device_id_type=MESH,
        )

    def p_copy(k):
        return pltpu.make_async_remote_copy(
            src_ref=pt_all.at[col], dst_ref=pt_all.at[col], send_sem=p_send.at[k], recv_sem=p_recv.at[col],
            device_id={"row": row, "col": (col + k) % n_col}, device_id_type=MESH,
        )

    def hop(c, p, way):
        to = [col + 2, col - 2, hi * 2 + 1 - lo][way]
        return pltpu.make_async_remote_copy(
            src_ref=piece(c, p), dst_ref=piece(c, p),
            send_sem=g_send.at[way, c, p], recv_sem=g_recv.at[c, p],
            device_id={"row": row, "col": to}, device_id_type=MESH,
        )

    def by_line(at, src, p):
        inner = ((at == 1) & (src == 0)) | ((at == outer - 2) & (src == outer - 1))
        edge = ((at == outer - 1) & (src == outer - 2)) | ((at == 0) & (src == 1))
        return (inner | edge) if p % 2 == 0 else inner

    def start_own_piece(p):
        @pl.when(hi + 1 < outer)
        def _():
            hop(col, p, 0).start()

        @pl.when(hi > 0)
        def _():
            hop(col, p, 1).start()

        hop(col, p, 2).start()

    for k in range(1, n_col):
        p_copy(k).start()
    assemble(0)
    start_own_piece(0)
    for k in [*range(2, n_row), 1]:
        pick(k)
        x_copy(k).start()

    er_at = fiota((1, LANE), 1)
    er_d = whole_part(er_at, ac)
    er_w = (rowf * ratio + er_d) * av + er_at - er_d * ac
    first = jnp.sum(jnp.where((wc == er_w) & (er_at < ar), NBF * rank_all + 1.0e6, 0.0), axis=0, keepdims=True) - 1.0e6
    u = fiota((live, LANE), 0) - first
    er = jnp.where((u >= 0.0) & (u < NBF), 1.0, 0.0).astype(BF)

    x_copy(1).wait_recv()
    assemble(1)
    start_own_piece(1)
    for k in range(1, n_col):
        src = (col + k) % n_col
        pltpu.make_async_copy(pt_all.at[src], pt_all.at[src], p_recv.at[src]).wait()
    mr[...] = mm_nt(er, pt_all[...].reshape(W, LANE)).astype(BF)

    slot_at = dc * slot + NBF * rank_slot
    mine = okc & (dc == colf)

    def process(c, p):
        i0, n = s_.starts[p], s_.sizes[p]
        lo_c = NBF * (nac - c.astype(F32) * ac)
        t = fiota((W, blk), 1) - lo_c
        hit = (t >= 0.0) & (t < NBF) & okc
        keep = mm(mr[i0 : i0 + n, :], jnp.where(hit, 1.0, 0.0).astype(BF))
        part = jnp.where(keep > 0.5, panel[c, i0 : i0 + n, :].astype(F32), 0.0)
        tot[...] += jnp.sum((part * part).reshape(n // 8, 8, blk), axis=0)
        part = part.astype(BF)
        to_slot = jnp.sum(jnp.where(hit, t + (slot_at + 1.0), 0.0), axis=0, keepdims=True) - 1.0
        to_new = jnp.sum(jnp.where(hit & mine, t + (NBF * vc + 1.0), 0.0), axis=0, keepdims=True) - 1.0
        left[c, i0 : i0 + n, :] = mm_nt(part, onehot(slots, to_slot)).astype(BF)
        racc[i0 : i0 + n, :] += mm_nt(part, onehot(blk, to_new))

    def arrived(c, p):
        pltpu.make_async_copy(piece(c, p), piece(c, p), g_recv.at[c, p]).wait()

    def gather(p):
        def step(d, _):
            for way in range(2):
                src = hi - d if way == 0 else hi + d
                ok = (d > 0) & (d < outer) & (src >= 0) & (src < outer)

                @pl.when(ok)
                def _():
                    c = src * 2 + lo
                    arrived(c, p)

                    @pl.when(hi + 1 < outer if way == 0 else hi > 0)
                    def _():
                        hop(c, p, way).start()

                    @pl.when(jnp.logical_not(by_line(hi, src, p)))
                    def _():
                        hop(c, p, 2).start()

            @pl.when(d == 1)
            def _():
                c = hi * 2 + 1 - lo
                arrived(c, p)

                @pl.when((hi + 1 < outer) & by_line(hi + 1, hi, p))
                def _():
                    hop(c, p, 0).start()

                @pl.when((hi > 0) & by_line(hi - 1, hi, p))
                def _():
                    hop(c, p, 1).start()

            def candidate(k, _):
                kind, way = k // 2, k % 2
                dist = d - kind
                src = hi + (1 - 2 * way) * dist
                ok = (dist >= 0) & (dist < outer) & (src >= 0) & (src < outer) & ((dist > 0) | (way == 0))

                @pl.when(ok)
                def _():
                    c = src * 2 + jnp.where(kind == 0, lo, 1 - lo)

                    @pl.when((kind == 1) & (dist > 0))
                    def _():
                        arrived(c, p)

                    process(c, p)

                return 0

            lax.fori_loop(0, 4, candidate, 0)
            return 0

        lax.fori_loop(0, outer + 1, step, 0)

    def part_of(r, ix):
        if ix < n_piece:
            return rt.at[r, pl.ds(s_.starts[ix], s_.sizes[ix]), :]
        return (sta, stb)[ix - n_piece].at[r, pl.ds(0, live), :]

    def share(ix):
        def send(r, to, sem):
            return pltpu.make_async_remote_copy(
                src_ref=part_of(r, ix), dst_ref=part_of(r, ix), send_sem=sem, recv_sem=r_recv.at[ix, r],
                device_id={"row": to, "col": col}, device_id_type=MESH,
            )

        return (
            [send(row, (x + k) % nx * 2 + core, r_send.at[ix, k]) for k in range(1, nx)]
            + [send(row, peer, r_send.at[ix, 0])],
            [send((x + k) % nx * 2 + core, peer, f_send.at[ix, k]) for k in range(1, nx)],
        )

    def start_share(ix):
        for cp in share(ix)[0]:
            cp.start()

    def got(ix, r):
        pltpu.make_async_copy(part_of(r, ix), part_of(r, ix), r_recv.at[ix, r]).wait()

    def relay(ix):
        onward = share(ix)[1]
        for k in range(1, nx):
            got(ix, (x + k) % nx * 2 + core)
            onward[k - 1].start()

    def finish(ix):
        for k in range(nx):
            got(ix, (x + k) % nx * 2 + 1 - core)

    def right_piece(p):
        i0, n = s_.starts[p], s_.sizes[p]
        rt[row, i0 : i0 + n, :] = racc[i0 : i0 + n, :].astype(BF)
        start_share(p)

    gather(0)
    for k in range(2, n_row):
        x_copy(k).wait_recv()
    for p in range(2, n_piece):
        assemble(p)
        start_own_piece(p)
    right_piece(0)
    gather(1)
    right_piece(1)
    relay(0)
    for r in range(n_row):
        ws = slice(r * ratio * av, (r + 1) * ratio * av)
        at = (dc[ws] - float(r * ratio)) * slots + bc[ws] * slot + NBF * rank_slot[ws]
        xm[r] = onehot(ratio * slots, expand(okc[ws], NBF * rank_all[ws], at, wide))
    my_new = NBF * ((dc - rowf * ratio) * ac + vc)
    fm[...] = onehot(s_.rows, expand(to_me, NBF * rank_all, my_new, wide))
    t = fiota((W, blk), 1) - NBF * vc
    kq[...] = mm(mr[...], jnp.where((t >= 0.0) & (t < NBF) & mine, 1.0, 0.0).astype(BF)).astype(BF)
    gather(2)
    right_piece(2)
    relay(1)
    gather(3)
    right_piece(3)

    def t_copy(k):
        return pltpu.make_async_remote_copy(
            src_ref=tot_all.at[row], dst_ref=tot_all.at[row], send_sem=t_send.at[k], recv_sem=t_recv.at[row],
            device_id={"row": (row + k) % n_row, "col": col}, device_id_type=MESH,
        )

    part_sum = tot[:, 0:LANE]
    for q in range(1, blk // LANE):
        part_sum += tot[:, q * LANE : (q + 1) * LANE]
    tot_all[row] = part_sum
    for k in range(1, n_row):
        t_copy(k).start()
    relay(2)
    for p in range(3):
        finish(p)
    relay(3)
    finish(3)
    for r in range(n_row):
        rx[r] = mm(xm[r], rt[r]).astype(BF)
    for k in range(1, n_row):
        src = (row + k) % n_row
        pltpu.make_async_copy(tot_all.at[src], tot_all.at[src], t_recv.at[src]).wait()
    total = jnp.sum(jnp.sum(tot_all[...], axis=0), axis=(0, 1), keepdims=True)
    scale = lax.rsqrt(total / order)
    half = live // 2

    def product(i0, j0, width):
        acc = None
        for c in range(n_col):
            b = jnp.concatenate(
                [
                    rx[d // ratio, (d % ratio) * slots + c * slot : (d % ratio) * slots + (c + 1) * slot, j0 : j0 + width]
                    for d in range(n_col)
                ],
                axis=0,
            )
            more = mm(left[c, i0 : i0 + half, :], b)
            acc = more if acc is None else acc + more
        return acc

    for q, (j0, width) in enumerate(s_.joff):
        st = (sta, stb)[q]
        for i0 in (0, half):
            square = product(i0, j0, width) * scale * scale
            keep = kq[i0 : i0 + half, j0 : j0 + width].astype(F32)
            st[row, i0 : i0 + half, :] = jnp.where(keep > 0.5, square, 0.0).astype(BF)
        start_share(n_piece + q)

    start = (rt[row].astype(F32) * scale).astype(BF)
    moved = 1.5 * mm(fm[...], start)
    out_ref[...] = moved[:, 0 : s_.cols]

    cac[live:, :] = jnp.zeros((wide - live, blk), BF)
    for q, (j0, width) in enumerate(s_.joff):
        st = (sta, stb)[q]
        relay(n_piece + q)
        finish(n_piece + q)
        for r in range(n_row):
            rx[r, :, j0 : j0 + width] = mm(xm[r], st[r]).astype(BF)
        for i0 in (0, half):
            cube = product(i0, j0, width) * scale
            keep = kq[i0 : i0 + half, j0 : j0 + width].astype(F32)
            cac[i0 : i0 + half, j0 : j0 + width] = jnp.where(keep > 0.5, cube, 0.0).astype(BF)
        done = mm(fm[...], cac[:, j0 : j0 + width])
        end = min(j0 + width, s_.cols)
        out_ref[:, j0:end] -= 0.5 * done[:, 0 : end - j0]

    for k in range(1, n_row):
        x_copy(k).wait_send()
        t_copy(k).wait_send()
    for k in range(1, n_col):
        p_copy(k).wait_send()
    for p in range(n_piece):

        def sent(q, _):
            c = q * 2 + lo

            @pl.when((q <= hi) & (hi + 1 < outer))
            def _():
                hop(c, p, 0).wait_send()

            @pl.when((q >= hi) & (hi > 0))
            def _():
                hop(c, p, 1).wait_send()

            @pl.when((q == hi) | jnp.logical_not(by_line(hi, q, p)))
            def _():
                hop(c, p, 2).wait_send()

            return 0

        lax.fori_loop(0, outer, sent, 0)
        c_other = hi * 2 + 1 - lo

        @pl.when((hi + 1 < outer) & by_line(hi + 1, hi, p))
        def _():
            hop(c_other, p, 0).wait_send()

        @pl.when((hi > 0) & by_line(hi - 1, hi, p))
        def _():
            hop(c_other, p, 1).wait_send()

    for ix in range(n_piece + 2):
        first, onward = share(ix)
        for cp in first + onward:
            cp.wait_send()


def on_device(hamiltonian, new_atom, pattern):
    rows, cols = hamiltonian.shape
    n_row, n_col = lax.axis_size("row"), lax.axis_size("col")
    ar, ac = pattern.shape
    s = Plan(n_row, n_col, rows, cols, ar, ac)
    vm = pl.BlockSpec(memory_space=pltpu.VMEM)
    dma = pltpu.SemaphoreType.DMA
    n_piece = len(s.sizes)
    slots = n_col * s.slot
    return pl.pallas_call(
        functools.partial(kernel, s, float(rows * n_row)),
        out_shape=jax.ShapeDtypeStruct((rows, cols), F32),
        in_specs=[pl.BlockSpec(memory_space=pl.ANY), vm, vm],
        out_specs=vm,
        scratch_shapes=[
            pltpu.VMEM((rows, cols), BF),
            pltpu.VMEM((s.wide, s.blk), BF),
            pltpu.VMEM((n_row - 1, s.sl, s.blk), BF),
            pltpu.VMEM((n_row - 1, s.slp, s.blk), BF),
            pltpu.VMEM((LANE, LANE), BF),
            pltpu.VMEM((n_col, s.av, LANE), BF),
            pltpu.VMEM((s.live, s.w), BF),
            pltpu.VMEM((s.live, s.blk), BF),
            pltpu.VMEM((n_col, s.live, s.blk), BF),
            pltpu.VMEM((n_col, s.live, slots), BF),
            pltpu.VMEM((s.live, s.blk), F32),
            pltpu.VMEM((n_row, s.wide, s.blk), BF),
            pltpu.VMEM((n_row, s.ratio * slots, s.blk), BF),
            pltpu.VMEM((n_row, s.ratio * slots, s.wide), BF),
            pltpu.VMEM((rows, s.wide), BF),
            pltpu.VMEM((n_row, s.wide, s.joff[0][1]), BF),
            pltpu.VMEM((n_row, s.wide, s.joff[1][1]), BF),
            pltpu.VMEM((s.wide, s.blk), BF),
            pltpu.VMEM((8, s.blk), F32),
            pltpu.VMEM((n_row, 8, LANE), F32),
            dma((1,)),
            dma((n_row,)),
            dma((n_row,)),
            dma((n_col,)),
            dma((n_col,)),
            dma((n_row,)),
            dma((n_row,)),
            dma((3, n_col, n_piece)),
            dma((n_col, n_piece)),
            dma((n_piece + 2, n_row)),
            dma((n_piece + 2, n_row)),
            dma((n_piece + 2, n_row)),
        ],
        compiler_params=pltpu.CompilerParams(
            collective_id=0, has_side_effects=True, vmem_limit_bytes=62 * 1024 * 1024
        ),
    )(hamiltonian, new_atom.reshape(1, -1), pattern)


def solution(mesh):
    in_specs = (P("row", "col"), P(), P("row", "col"))
    out_specs = P("row", "col")
    return jax.shard_map(
        on_device, mesh=mesh, in_specs=in_specs, out_specs=out_specs, check_vma=False
    )
```

```python
import functools

import jax
import jax.numpy as jnp
import numpy as np
from jax import lax
from jax.experimental import pallas as pl
from jax.experimental.pallas import tpu as pltpu
from jax.sharding import PartitionSpec as P

NBF = 13
LANE = 128
BF = jnp.bfloat16
F32 = jnp.float32
I32 = jnp.int32
MESH = pl.DeviceIdType.MESH
FAR = -1.0e6


def up(n, k):
    return -(-n // k) * k


def mm(a, b):
    return jnp.dot(a, b, preferred_element_type=F32)


def mm_nt(a, b):
    return lax.dot_general(a, b, (((1,), (1,)), ((), ())), preferred_element_type=F32)


def iota(shape, axis):
    return lax.broadcasted_iota(I32, shape, axis)


def fiota(shape, axis):
    return iota(shape, axis).astype(F32)


def whole_part(x, n):
    return jnp.floor((x + 0.5) * (1.0 / n))


def expand(sel, lo, start, size):
    u = fiota((lo.shape[0], size), 1) - lo
    hit = sel & (u >= 0.0) & (u < NBF)
    return jnp.sum(jnp.where(hit, u + (start + 1.0), 0.0), axis=0, keepdims=True) - 1.0


def onehot(rows, places, offset=0):
    i = fiota((rows, places.shape[1]), 0) + float(offset)
    return jnp.where(i == places, 1.0, 0.0).astype(BF)


class Plan:
    def __init__(self, n_row, n_col, rows, cols, ar, ac):
        self.n_row, self.n_col, self.rows, self.cols, self.ar, self.ac = n_row, n_col, rows, cols, ar, ac
        self.ratio = n_col // n_row
        self.nx = n_row // 2
        self.outer = n_col // 2
        self.av = up(ac, 16)
        self.w = n_col * self.av
        self.blk = up(cols, LANE)
        self.live = up(rows, 16)
        self.wide = up(rows, LANE)
        count = np.bincount((1 + np.arange(ac)) % n_col, minlength=n_col)
        self.slot = up(int(count.max()) * NBF, 16)
        r = self.ratio
        pair = [
            sum(int(count[(r * k + g - b) % n_col]) for b in range(r) for g in range(r)) for k in range(n_row)
        ]
        self.sl = up(max(pair) * NBF, 16)
        self.slp = up(self.sl, LANE)
        own = pair[0] * NBF // 16 * 16
        chip = (pair[0] + min(pair[1], pair[n_row - 1])) * NBF // 16 * 16
        rest = self.live - chip
        last = up(rest // 4, 16)
        mid = up((rest - last) // 2, 16)
        ends = [0, own, chip, chip + mid, self.live - last, self.live]
        self.starts, self.sizes = ends[:-1], [b - a for a, b in zip(ends, ends[1:])]
        self.groups = [[0, 1], [2, 3], [4]]
        self.spans = [(ends[g[0]], ends[g[-1] + 1]) for g in self.groups]
        self.stored = n_row * self.ratio * n_col * self.slot * self.wide * 2 <= 8 * 1024 * 1024
        self.joff = [(0, self.blk - LANE), (self.blk - LANE, LANE)]


def kernel(
    s_, order, h_ref, na_ref, pat_ref, out_ref,
    hp, xs, rin, pp, pt_all, mr, kq, panel, left, pos, pull, rt, rx, xm, fm, sta, stb, cac, tot, tot_all,
    x_send, x_recv, p_send, p_recv, t_send, t_recv, g_send, g_recv, r_send, r_recv, f_send,
):
    n_row, n_col, ratio, nx, outer = s_.n_row, s_.n_col, s_.ratio, s_.nx, s_.outer
    ac, ar, av, W, blk, live, wide = s_.ac, s_.ar, s_.av, s_.w, s_.blk, s_.live, s_.wide
    slot, sl, slp = s_.slot, s_.sl, s_.slp
    row = lax.axis_index("row")
    col = lax.axis_index("col")
    hi, lo = col // 2, col % 2
    x, core = row // 2, row % 2
    peer = x * 2 + 1 - core
    n_piece = len(s_.sizes)
    n_group = len(s_.groups)
    slots = n_col * slot

    barrier = pltpu.get_barrier_semaphore()
    for k in range(1, n_row):
        pl.semaphore_signal(barrier, inc=1, device_id={"row": (row + k) % n_row, "col": col}, device_id_type=MESH)
    for k in range(1, n_col):
        pl.semaphore_signal(barrier, inc=1, device_id={"row": row, "col": (col + k) % n_col}, device_id_type=MESH)

    rowf, colf, xf, coref, peerf = [i.astype(F32) for i in (row, col, x, core, peer)]

    def places(w):
        d = whole_part(w, av)
        v = w - d * av
        return d, v, v < ac

    def source(na, d):
        b = whole_part(na, ac)
        src = whole_part(b, ratio)
        home = whole_part(d, ratio)
        far = jnp.where(whole_part(src, 2) == whole_part(home, 2), 1.0, 2.0)
        return b, src, home, jnp.where(src == home, 0.0, far)

    wc, wr = fiota((W, 1), 0), fiota((1, W), 1)
    dc, vc, okc = places(wc)
    dr, vr, okr = places(wr)
    atoms = na_ref[...].astype(F32)
    here = (fiota((W, atoms.shape[1]), 1) == dc * ac + vc) & okc
    nac = jnp.where(okc, jnp.sum(jnp.where(here, atoms, 0.0), axis=1, keepdims=True), -1.0e5)
    nar = jnp.sum(jnp.where(fiota((W, W), 0) == wr, nac, 0.0), axis=0, keepdims=True)
    bc, srcc, homec, grpc = source(nac, dc)
    br, srcr, homer, grpr = source(nar, dr)
    before = wr < wc

    def rank(hit):
        return jnp.sum(jnp.where(hit & okr, 1.0, 0.0), axis=1, keepdims=True)

    rank_slot = rank((dr == dc) & (br == bc) & before)
    rank_pair = rank((homer == homec) & (srcr == srcc) & before)
    rank_all = rank((homer == homec) & ((grpr < grpc) | ((grpr == grpc) & before)))
    old_at = NBF * (nac - srcc * ar)
    kx = whole_part(homec, 2) - xf
    kx = jnp.where(kx < 0.0, kx + nx, kx)
    kc = homec - 2.0 * whole_part(homec, 2)
    kc = jnp.where(kc == coref, 0.0, 1.0)
    from_me = okc & (srcc == rowf)
    to_me = okc & (homec == rowf)
    out_place = expand(from_me, old_at, (2.0 * kx + kc) * slp + NBF * rank_pair, wide)
    own_place = expand(from_me & to_me, old_at, NBF * rank_all, wide)

    def other(sign, k):
        return ((x + sign * (k // 2) + nx) % nx) * 2 + (core + k % 2) % 2

    in_place = {
        k: expand(to_me & (srcc == other(-1, k).astype(F32)), NBF * rank_pair, NBF * rank_all, slp)
        for k in range(1, n_row)
    }

    pp[...] = jnp.zeros_like(pp)
    pp[0:ac, 0:ar] = pat_ref[...].astype(F32)
    pt_all[col] = pp[...].astype(BF)
    hp[...] = jnp.zeros_like(hp)
    rin[:, sl:, :] = jnp.zeros((n_row - 1, slp - sl, blk), BF)
    rt[:, live:, :] = jnp.zeros((n_row, wide - live, blk), BF)
    sta[:, live:, :] = jnp.zeros((n_row, wide - live, sta.shape[2]), BF)
    stb[:, live:, :] = jnp.zeros((n_row, wide - live, stb.shape[2]), BF)
    tot[...] = jnp.zeros_like(tot)
    hp[0 : s_.rows, 0 : s_.cols] = h_ref[...]

    def pick(k):
        xs[k - 1] = mm(onehot(sl, out_place, k * slp), hp[...]).astype(BF)

    def piece(c, p):
        return panel.at[c, pl.ds(s_.starts[p], s_.sizes[p]), :]

    def assemble(p):
        i0, n = s_.starts[p], s_.sizes[p]
        part = None
        if p < 2:
            part = mm(onehot(n, own_place, i0), hp[...])
        for k in range(1, n_row):
            if p >= (1 if k == 1 else 2):
                more = mm(onehot(n, in_place[k], i0), rin[k - 1])
                part = more if part is None else part + more
        panel[col, i0 : i0 + n, :] = part.astype(BF)

    pl.semaphore_wait(barrier, n_row + n_col - 2)

    def x_copy(k):
        return pltpu.make_async_remote_copy(
            src_ref=xs.at[k - 1], dst_ref=rin.at[k - 1, pl.ds(0, sl), :],
            send_sem=x_send.at[k], recv_sem=x_recv.at[k],
            device_id={"row": other(1, k), "col": col}, device_id_type=MESH,
        )

    def p_copy(k):
        return pltpu.make_async_remote_copy(
            src_ref=pt_all.at[col], dst_ref=pt_all.at[col], send_sem=p_send.at[k], recv_sem=p_recv.at[col],
            device_id={"row": row, "col": (col + k) % n_col}, device_id_type=MESH,
        )

    def hop(c, p, way):
        to = [col + 2, col - 2, hi * 2 + 1 - lo][way]
        return pltpu.make_async_remote_copy(
            src_ref=piece(c, p), dst_ref=piece(c, p),
            send_sem=g_send.at[way, c, p], recv_sem=g_recv.at[c, p],
            device_id={"row": row, "col": to}, device_id_type=MESH,
        )

    def by_line(at, src, p):
        inner = ((at == 1) & (src == 0)) | ((at == outer - 2) & (src == outer - 1))
        edge = ((at == outer - 1) & (src == outer - 2)) | ((at == 0) & (src == 1))
        return (inner | edge) if p in (0, 2) else inner

    def start_own_piece(p):
        @pl.when(hi + 1 < outer)
        def _():
            hop(col, p, 0).start()

        @pl.when(hi > 0)
        def _():
            hop(col, p, 1).start()

        hop(col, p, 2).start()

    for k in range(1, n_col):
        p_copy(k).start()
    assemble(0)
    start_own_piece(0)
    for k in [*range(2, n_row), 1]:
        pick(k)
        x_copy(k).start()

    er_at = fiota((1, LANE), 1)
    er_d = whole_part(er_at, ac)
    er_w = (rowf * ratio + er_d) * av + er_at - er_d * ac
    first = jnp.sum(jnp.where((wc == er_w) & (er_at < ar), NBF * rank_all + 1.0e6, 0.0), axis=0, keepdims=True) - 1.0e6
    u = fiota((live, LANE), 0) - first
    er = jnp.where((u >= 0.0) & (u < NBF), 1.0, 0.0).astype(BF)

    x_copy(1).wait_recv()
    assemble(1)
    start_own_piece(1)
    for k in range(1, n_col):
        src = (col + k) % n_col
        pltpu.make_async_copy(pt_all.at[src], pt_all.at[src], p_recv.at[src]).wait()
    mr[...] = mm_nt(er, pt_all[...].reshape(W, LANE)).astype(BF)

    mine = okc & (dc == colf)
    coded = jnp.broadcast_to(jnp.where(okc, dc * 8.0 + rank_slot + 1.0, 0.0), (W, LANE)).astype(BF)

    def atom_of(t):
        return jnp.where(t < s_.cols, whole_part(t, NBF), -1.0e4)

    atom_c, atom_r = atom_of(fiota((blk, 1), 0)), atom_of(fiota((1, blk), 1))
    within = fiota((blk, 1), 0) - NBF * atom_c
    my_tile = pl.multiple_of(col * slot // LANE * LANE, LANE)
    my_lane = (col * slot % LANE).astype(F32)
    pull_place = expand(mine, NBF * vc, bc * LANE + my_lane + NBF * rank_slot, blk)

    def chunk_tables(c, _):
        code = mm(jnp.where(nar - (c * ac).astype(F32) == atom_c, 1.0, 0.0).astype(BF), coded) - 1.0
        far = jnp.floor(code * 0.125)
        at = far * slot + NBF * (code - 8.0 * far) + within
        pos[c] = jnp.where(code < 0.0, -1.0, at)
        rows = pl.ds(pl.multiple_of(c * LANE, LANE), LANE)
        pull[rows, :] = onehot(LANE, pull_place - (c * LANE).astype(F32))
        return 0

    lax.fori_loop(0, n_col, chunk_tables, 0)

    def process(c, g):
        i0, i1 = s_.spans[g]
        n = i1 - i0
        hit = jnp.where(nac - c.astype(F32) * ac == atom_r, 1.0, 0.0).astype(BF)
        keep = mm(mr[i0:i1, :], hit)
        part = jnp.where(keep > 0.5, panel[c, i0:i1, :].astype(F32), 0.0)
        tot[...] += jnp.sum((part * part).reshape(n // 8, 8, blk), axis=0)
        at = pos[c]
        lane = fiota((blk, LANE), 1)
        to_slot = jnp.concatenate(
            [jnp.where(lane + float(q) == at, 1.0, 0.0).astype(BF) for q in range(0, slots, LANE)], axis=1
        )
        left[i0:i1, pl.ds(pl.multiple_of(c * slots, slots), slots)] = mm(part.astype(BF), to_slot).astype(BF)

    def arrived(c, p):
        pltpu.make_async_copy(piece(c, p), piece(c, p), g_recv.at[c, p]).wait()

    def forward(d, g):
        for way in range(2):
            src = hi - d if way == 0 else hi + d

            @pl.when((src >= 0) & (src < outer))
            def _():
                c = src * 2 + lo
                for p in s_.groups[g]:
                    arrived(c, p)

                    @pl.when(hi + 1 < outer if way == 0 else hi > 0)
                    def _():
                        hop(c, p, way).start()

                    @pl.when(jnp.logical_not(by_line(hi, src, p)))
                    def _():
                        hop(c, p, 2).start()

        @pl.when(d == 1)
        def _():
            c = hi * 2 + 1 - lo
            for p in s_.groups[g]:
                arrived(c, p)

                @pl.when((hi + 1 < outer) & by_line(hi + 1, hi, p))
                def _():
                    hop(c, p, 0).start()

                @pl.when((hi > 0) & by_line(hi - 1, hi, p))
                def _():
                    hop(c, p, 1).start()

    def work(e, g):
        def candidate(k, _):
            kind, way = k // 2, k % 2
            dist = e - 1 - kind
            src = hi + (1 - 2 * way) * dist
            ok = (dist >= 0) & (dist < outer) & (src >= 0) & (src < outer) & ((dist > 0) | (way == 0))

            @pl.when(ok)
            def _():
                c = src * 2 + jnp.where(kind == 0, lo, 1 - lo)

                @pl.when((kind == 1) & (dist > 0))
                def _():
                    for p in s_.groups[g]:
                        arrived(c, p)

                process(c, g)

            return 0

        lax.fori_loop(0, 4, candidate, 0)

    def gather(g, between):
        def step(d, _):
            forward(d, g)
            for at, extra in between.items():
                pl.when(d == at)(extra)
            if g > 0:

                @pl.when(d <= 2)
                def _():
                    work(outer - 1 + d, g - 1)

                @pl.when(d == 2)
                def _():
                    right_share(g - 1)

            work(d, g)
            return 0

        lax.fori_loop(1, outer, step, 0)

    def part_of(r, ix):
        if ix < n_group:
            i0, i1 = s_.spans[ix]
            return rt.at[r, pl.ds(i0, i1 - i0), :]
        return (sta, stb)[ix - n_group].at[r, pl.ds(0, live), :]

    def share(ix):
        def send(r, to, sem):
            return pltpu.make_async_remote_copy(
                src_ref=part_of(r, ix), dst_ref=part_of(r, ix), send_sem=sem, recv_sem=r_recv.at[ix, r],
                device_id={"row": to, "col": col}, device_id_type=MESH,
            )

        return (
            [send(row, (x + k) % nx * 2 + core, r_send.at[ix, k]) for k in range(1, nx)]
            + [send(row, peer, r_send.at[ix, 0])],
            [send((x + k) % nx * 2 + core, peer, f_send.at[ix, k]) for k in range(1, nx)],
        )

    def start_share(ix):
        for cp in share(ix)[0]:
            cp.start()

    def got(ix, r):
        pltpu.make_async_copy(part_of(r, ix), part_of(r, ix), r_recv.at[ix, r]).wait()

    def relay(ix):
        onward = share(ix)[1]
        for k in range(1, nx):
            got(ix, (x + k) % nx * 2 + core)
            onward[k - 1].start()

    def finish(ix):
        for k in range(nx):
            got(ix, (x + k) % nx * 2 + 1 - core)

    def right_share(g):
        i0, i1 = s_.spans[g]
        mine_first = jnp.concatenate([left[i0:i1, pl.ds(c * slots + my_tile, LANE)] for c in range(n_col)], axis=1)
        rt[row, i0:i1, :] = mm(mine_first, pull[...]).astype(BF)
        start_share(g)

    def later_rows():
        for k in range(2, n_row):
            x_copy(k).wait_recv()
        for p in range(2, n_piece):
            assemble(p)
            start_own_piece(p)

    def row_places(r):
        ws = slice(r * ratio * av, (r + 1) * ratio * av)
        at = (dc[ws] - float(r * ratio)) * slots + bc[ws] * slot + NBF * rank_slot[ws]
        return expand(okc[ws], NBF * rank_all[ws], at, wide)

    def row_slots(r, a, b):
        return xm[r, :, a:b] if s_.stored else onehot(ratio * slots, xm[r, 0:1, a:b])

    def row_blocks(visit):
        if s_.stored:
            for r in range(n_row):
                visit(r)
        else:
            lax.fori_loop(0, n_row, lambda r, _: (visit(r), 0)[1], 0)

    def tables():
        for r in range(n_row):
            at = row_places(r)
            xm[r] = onehot(ratio * slots, at) if s_.stored else jnp.broadcast_to(at, (8, wide))
        my_new = NBF * ((dc - rowf * ratio) * ac + vc)
        fm[...] = onehot(s_.rows, expand(to_me, NBF * rank_all, my_new, wide))
        t = fiota((W, blk), 1) - NBF * vc
        kq[...] = mm(mr[...], jnp.where((t >= 0.0) & (t < NBF) & mine, 1.0, 0.0).astype(BF)).astype(BF)

    gather(0, {2: later_rows})
    gather(1, {1: tables})
    gather(2, {1: lambda: relay(0)})
    last = n_group - 1

    def tail(e, _):
        work(e, last)
        return 0

    lax.fori_loop(outer, outer + 2, tail, 0)
    right_share(last)
    relay(1)

    def t_copy(k):
        return pltpu.make_async_remote_copy(
            src_ref=tot_all.at[row], dst_ref=tot_all.at[row], send_sem=t_send.at[k], recv_sem=t_recv.at[row],
            device_id={"row": (row + k) % n_row, "col": col}, device_id_type=MESH,
        )

    part_sum = tot[:, 0:LANE]
    for q in range(1, blk // LANE):
        part_sum += tot[:, q * LANE : (q + 1) * LANE]
    tot_all[row] = part_sum
    for k in range(1, n_row):
        t_copy(k).start()
    finish(0)
    finish(1)
    early = s_.spans[2][0] // LANE * LANE

    def spread(r, rows, j0, width, add):
        for q in range(n_col * ratio):
            at = pl.ds(r * ratio * slot + q % n_col * slots + q // n_col * slot, slot)
            if not s_.stored:
                at = pl.ds(pl.multiple_of(at.start, slot), slot)
            part = rows[q * slot : (q + 1) * slot].astype(BF)
            if add:
                rx[at, j0 : j0 + width] += part
            else:
                rx[at, j0 : j0 + width] = part

    row_blocks(lambda r: spread(r, mm(row_slots(r, 0, early), rt[r, 0:early, :]), 0, blk, False))
    relay(2)
    finish(2)
    row_blocks(lambda r: spread(r, mm(row_slots(r, early, wide), rt[r, early:, :]), 0, blk, True))
    for k in range(1, n_row):
        src = (row + k) % n_row
        pltpu.make_async_copy(tot_all.at[src], tot_all.at[src], t_recv.at[src]).wait()
    total = jnp.sum(jnp.sum(tot_all[...], axis=0), axis=(0, 1), keepdims=True)
    scale = lax.rsqrt(total / order)

    half = live // 2

    def product(i0, j0, width):
        depth = min(n_col * slots, 4096)
        if depth == n_col * slots:
            return mm(left[i0 : i0 + half, :], rx[:, j0 : j0 + width])

        def more(q, acc):
            k = pl.ds(pl.multiple_of(q * slots, slots), slots)
            return acc + mm(left[i0 : i0 + half, k], rx[k, j0 : j0 + width])

        return lax.fori_loop(0, n_col, more, jnp.zeros((half, width), F32))

    for q, (j0, width) in enumerate(s_.joff):
        st = (sta, stb)[q]
        for i0 in (0, half):
            square = product(i0, j0, width) * scale * scale
            keep = kq[i0 : i0 + half, j0 : j0 + width].astype(F32)
            st[row, i0 : i0 + half, :] = jnp.where(keep > 0.5, square, 0.0).astype(BF)
        start_share(n_group + q)

    start = (rt[row].astype(F32) * scale).astype(BF)
    moved = 1.5 * mm(fm[...], start)
    out_ref[...] = moved[:, 0 : s_.cols]

    for k in range(1, n_row):
        x_copy(k).wait_send()
        t_copy(k).wait_send()
    for k in range(1, n_col):
        p_copy(k).wait_send()
    for p in range(n_piece):

        def sent(q, _):
            c = q * 2 + lo

            @pl.when((q <= hi) & (hi + 1 < outer))
            def _():
                hop(c, p, 0).wait_send()

            @pl.when((q >= hi) & (hi > 0))
            def _():
                hop(c, p, 1).wait_send()

            @pl.when((q == hi) | jnp.logical_not(by_line(hi, q, p)))
            def _():
                hop(c, p, 2).wait_send()

            return 0

        lax.fori_loop(0, outer, sent, 0)
        c_other = hi * 2 + 1 - lo

        @pl.when((hi + 1 < outer) & by_line(hi + 1, hi, p))
        def _():
            hop(c_other, p, 0).wait_send()

        @pl.when((hi > 0) & by_line(hi - 1, hi, p))
        def _():
            hop(c_other, p, 1).wait_send()

    def sent_share(ix):
        first, onward = share(ix)
        for cp in first + onward:
            cp.wait_send()

    for ix in range(n_group):
        sent_share(ix)

    cac[live:, :] = jnp.zeros((wide - live, blk), BF)
    for q, (j0, width) in enumerate(s_.joff):
        st = (sta, stb)[q]
        relay(n_group + q)
        finish(n_group + q)
        row_blocks(lambda r: spread(r, mm(row_slots(r, 0, wide), st[r]), j0, width, False))
        for i0 in (0, half):
            cube = product(i0, j0, width) * scale
            keep = kq[i0 : i0 + half, j0 : j0 + width].astype(F32)
            cac[i0 : i0 + half, j0 : j0 + width] = jnp.where(keep > 0.5, cube, 0.0).astype(BF)
        done = mm(fm[...], cac[:, j0 : j0 + width])
        end = min(j0 + width, s_.cols)
        out_ref[:, j0:end] -= 0.5 * done[:, 0 : end - j0]

    for q in range(2):
        sent_share(n_group + q)


def on_device(hamiltonian, new_atom, pattern):
    rows, cols = hamiltonian.shape
    n_row, n_col = lax.axis_size("row"), lax.axis_size("col")
    ar, ac = pattern.shape
    s = Plan(n_row, n_col, rows, cols, ar, ac)
    vm = pl.BlockSpec(memory_space=pltpu.VMEM)
    dma = pltpu.SemaphoreType.DMA
    n_piece = len(s.sizes)
    n_group = len(s.groups)
    slots = n_col * s.slot
    buffers = [
        pltpu.VMEM((s.wide, s.blk), BF),
        pltpu.VMEM((n_row - 1, s.sl, s.blk), BF),
        pltpu.VMEM((n_row - 1, s.slp, s.blk), BF),
        pltpu.VMEM((s.av, LANE), F32),
        pltpu.VMEM((n_col, s.av, LANE), BF),
        pltpu.VMEM((s.live, s.w), BF),
        pltpu.VMEM((s.live, s.blk), BF),
        pltpu.VMEM((n_col, s.live, s.blk), BF),
        pltpu.VMEM((s.live, n_col * slots), BF),
        pltpu.VMEM((n_col, s.blk, LANE), F32),
        pltpu.VMEM((n_col * LANE, s.blk), BF),
        pltpu.VMEM((n_row, s.wide, s.blk), BF),
        pltpu.VMEM((n_col * slots, s.blk), BF),
        pltpu.VMEM((n_row, s.ratio * slots, s.wide) if s.stored else (n_row, 8, s.wide), BF if s.stored else F32),
        pltpu.VMEM((rows, s.wide), BF),
        pltpu.VMEM((n_row, s.wide, s.joff[0][1]), BF),
        pltpu.VMEM((n_row, s.wide, s.joff[1][1]), BF),
        pltpu.VMEM((s.wide, s.blk), BF),
        pltpu.VMEM((8, s.blk), F32),
        pltpu.VMEM((n_row, 8, LANE), F32),
    ]
    held = sum(int(np.prod(b.shape)) * np.dtype(b.dtype).itemsize for b in buffers)
    return pl.pallas_call(
        functools.partial(kernel, s, float(rows * n_row)),
        out_shape=jax.ShapeDtypeStruct((rows, cols), F32),
        in_specs=[vm, vm, vm],
        out_specs=vm,
        scratch_shapes=[
            *buffers,
            dma((n_row,)),
            dma((n_row,)),
            dma((n_col,)),
            dma((n_col,)),
            dma((n_row,)),
            dma((n_row,)),
            dma((3, n_col, n_piece)),
            dma((n_col, n_piece)),
            dma((n_group + 2, n_row)),
            dma((n_group + 2, n_row)),
            dma((n_group + 2, n_row)),
        ],
        compiler_params=pltpu.CompilerParams(
            collective_id=0, has_side_effects=True, vmem_limit_bytes=min(held + held // 8 + 7 * 1024 * 1024, 62 * 1024 * 1024)
        ),
    )(hamiltonian, new_atom.reshape(1, -1), pattern.T)


def solution(mesh):
    in_specs = (P("row", "col"), P(), P("row", "col"))
    out_specs = P("row", "col")
    return jax.shard_map(
        on_device, mesh=mesh, in_specs=in_specs, out_specs=out_specs, check_vma=False
    )
```

```python
import functools

import jax
import jax.numpy as jnp
import numpy as np
from jax import lax
from jax.experimental import pallas as pl
from jax.experimental.pallas import tpu as pltpu
from jax.sharding import PartitionSpec as P

NBF = 13
LANE = 128
BF = jnp.bfloat16
F32 = jnp.float32
I32 = jnp.int32
MESH = pl.DeviceIdType.MESH
FAR = -1.0e6


def up(n, k):
    return -(-n // k) * k


def mm(a, b):
    return jnp.dot(a, b, preferred_element_type=F32)


def mm_nt(a, b):
    return lax.dot_general(a, b, (((1,), (1,)), ((), ())), preferred_element_type=F32)


def iota(shape, axis):
    return lax.broadcasted_iota(I32, shape, axis)


def fiota(shape, axis):
    return iota(shape, axis).astype(F32)


def whole_part(x, n):
    return jnp.floor((x + 0.5) * (1.0 / n))


def expand(sel, lo, start, size):
    u = fiota((lo.shape[0], size), 1) - lo
    hit = sel & (u >= 0.0) & (u < NBF)
    return jnp.sum(jnp.where(hit, u + (start + 1.0), 0.0), axis=0, keepdims=True) - 1.0


def onehot(rows, places, offset=0):
    i = fiota((rows, places.shape[1]), 0) + float(offset)
    return jnp.where(i == places, 1.0, 0.0).astype(BF)


class Plan:
    def __init__(self, n_row, n_col, rows, cols, ar, ac):
        self.n_row, self.n_col, self.rows, self.cols, self.ar, self.ac = n_row, n_col, rows, cols, ar, ac
        self.ratio = n_col // n_row
        self.nx = n_row // 2
        self.outer = n_col // 2
        self.av = up(ac, 16)
        self.w = n_col * self.av
        self.blk = up(cols, LANE)
        self.live = up(rows, 16)
        self.wide = up(rows, LANE)
        count = np.bincount((1 + np.arange(ac)) % n_col, minlength=n_col)
        self.slot = up(int(count.max()) * NBF, 16)
        r = self.ratio
        pair = [
            sum(int(count[(r * k + g - b) % n_col]) for b in range(r) for g in range(r)) for k in range(n_row)
        ]
        self.sl = up(max(pair) * NBF, 16)
        self.slp = up(self.sl, LANE)
        own = pair[0] * NBF // 16 * 16
        chip = (pair[0] + min(pair[1], pair[n_row - 1])) * NBF // 16 * 16
        rest = self.live - chip
        last = up(rest // 3, 16)
        mid = up((rest - last) // 2, 16)
        ends = [0, own, chip, chip + mid, self.live - last, self.live]
        self.starts, self.sizes = ends[:-1], [b - a for a, b in zip(ends, ends[1:])]
        self.groups = [[0, 1], [2, 3], [4]]
        self.spans = [(ends[g[0]], ends[g[-1] + 1]) for g in self.groups]
        self.stored = n_row * self.ratio * n_col * self.slot * self.wide * 2 <= 8 * 1024 * 1024
        self.joff = [(0, self.blk - LANE), (self.blk - LANE, LANE)]


def kernel(
    s_, order, h_ref, na_ref, pat_ref, out_ref,
    hp, xs, rin, pp, pt_all, mr, kq, panel, left, pos, pull, rt, rx, xm, fm, sta, stb, cac, tot, tot_all,
    x_send, x_recv, p_send, p_recv, t_send, t_recv, g_send, g_recv, r_send, r_recv, f_send,
):
    n_row, n_col, ratio, nx, outer = s_.n_row, s_.n_col, s_.ratio, s_.nx, s_.outer
    ac, ar, av, W, blk, live, wide = s_.ac, s_.ar, s_.av, s_.w, s_.blk, s_.live, s_.wide
    slot, sl, slp = s_.slot, s_.sl, s_.slp
    row = lax.axis_index("row")
    col = lax.axis_index("col")
    hi, lo = col // 2, col % 2
    x, core = row // 2, row % 2
    peer = x * 2 + 1 - core
    n_piece = len(s_.sizes)
    n_group = len(s_.groups)
    slots = n_col * slot

    barrier = pltpu.get_barrier_semaphore()
    for k in range(1, n_row):
        pl.semaphore_signal(barrier, inc=1, device_id={"row": (row + k) % n_row, "col": col}, device_id_type=MESH)
    for k in range(1, n_col):
        pl.semaphore_signal(barrier, inc=1, device_id={"row": row, "col": (col + k) % n_col}, device_id_type=MESH)

    rowf, colf, xf, coref, peerf = [i.astype(F32) for i in (row, col, x, core, peer)]

    def places(w):
        d = whole_part(w, av)
        v = w - d * av
        return d, v, v < ac

    def source(na, d):
        b = whole_part(na, ac)
        src = whole_part(b, ratio)
        home = whole_part(d, ratio)
        far = jnp.where(whole_part(src, 2) == whole_part(home, 2), 1.0, 2.0)
        return b, src, home, jnp.where(src == home, 0.0, far)

    wc, wr = fiota((W, 1), 0), fiota((1, W), 1)
    dc, vc, okc = places(wc)
    dr, vr, okr = places(wr)
    atoms = na_ref[...].astype(F32)
    here = (fiota((W, atoms.shape[1]), 1) == dc * ac + vc) & okc
    nac = jnp.where(okc, jnp.sum(jnp.where(here, atoms, 0.0), axis=1, keepdims=True), -1.0e5)
    nar = jnp.sum(jnp.where(fiota((W, W), 0) == wr, nac, 0.0), axis=0, keepdims=True)
    bc, srcc, homec, grpc = source(nac, dc)
    br, srcr, homer, grpr = source(nar, dr)
    before = wr < wc

    def rank(hit):
        return jnp.sum(jnp.where(hit & okr, 1.0, 0.0), axis=1, keepdims=True)

    rank_slot = rank((dr == dc) & (br == bc) & before)
    rank_pair = rank((homer == homec) & (srcr == srcc) & before)
    rank_all = rank((homer == homec) & ((grpr < grpc) | ((grpr == grpc) & before)))
    old_at = NBF * (nac - srcc * ar)
    kx = whole_part(homec, 2) - xf
    kx = jnp.where(kx < 0.0, kx + nx, kx)
    kc = homec - 2.0 * whole_part(homec, 2)
    kc = jnp.where(kc == coref, 0.0, 1.0)
    from_me = okc & (srcc == rowf)
    to_me = okc & (homec == rowf)
    out_place = expand(from_me, old_at, (2.0 * kx + kc) * slp + NBF * rank_pair, wide)
    own_place = expand(from_me & to_me, old_at, NBF * rank_all, wide)

    def other(sign, k):
        return ((x + sign * (k // 2) + nx) % nx) * 2 + (core + k % 2) % 2

    in_place = {
        k: expand(to_me & (srcc == other(-1, k).astype(F32)), NBF * rank_pair, NBF * rank_all, slp)
        for k in range(1, n_row)
    }

    pp[...] = jnp.zeros_like(pp)
    pp[0:ac, 0:ar] = pat_ref[...].astype(F32)
    pt_all[col] = pp[...].astype(BF)
    hp[...] = jnp.zeros_like(hp)
    rin[:, sl:, :] = jnp.zeros((n_row - 1, slp - sl, blk), BF)
    rt[:, live:, :] = jnp.zeros((n_row, wide - live, blk), BF)
    sta[:, live:, :] = jnp.zeros((n_row, wide - live, sta.shape[2]), BF)
    stb[:, live:, :] = jnp.zeros((n_row, wide - live, stb.shape[2]), BF)
    tot[...] = jnp.zeros_like(tot)
    hp[0 : s_.rows, 0 : s_.cols] = h_ref[...]

    def pick(k):
        xs[k - 1] = mm(onehot(sl, out_place, k * slp), hp[...]).astype(BF)

    def piece(c, p):
        return panel.at[c, pl.ds(s_.starts[p], s_.sizes[p]), :]

    def assemble(p):
        i0, n = s_.starts[p], s_.sizes[p]
        part = None
        if p < 2:
            part = mm(onehot(n, own_place, i0), hp[...])
        for k in range(1, n_row):
            if p >= (1 if k == 1 else 2):
                more = mm(onehot(n, in_place[k], i0), rin[k - 1])
                part = more if part is None else part + more
        panel[col, i0 : i0 + n, :] = part.astype(BF)

    pl.semaphore_wait(barrier, n_row + n_col - 2)

    def x_copy(k):
        return pltpu.make_async_remote_copy(
            src_ref=xs.at[k - 1], dst_ref=rin.at[k - 1, pl.ds(0, sl), :],
            send_sem=x_send.at[k], recv_sem=x_recv.at[k],
            device_id={"row": other(1, k), "col": col}, device_id_type=MESH,
        )

    def p_copy(k):
        return pltpu.make_async_remote_copy(
            src_ref=pt_all.at[col], dst_ref=pt_all.at[col], send_sem=p_send.at[k], recv_sem=p_recv.at[col],
            device_id={"row": row, "col": (col + k) % n_col}, device_id_type=MESH,
        )

    def hop(c, p, way):
        to = [col + 2, col - 2, hi * 2 + 1 - lo][way]
        return pltpu.make_async_remote_copy(
            src_ref=piece(c, p), dst_ref=piece(c, p),
            send_sem=g_send.at[way, c, p], recv_sem=g_recv.at[c, p],
            device_id={"row": row, "col": to}, device_id_type=MESH,
        )

    def by_line(at, src, p):
        inner = ((at == 1) & (src == 0)) | ((at == outer - 2) & (src == outer - 1))
        edge = ((at == outer - 1) & (src == outer - 2)) | ((at == 0) & (src == 1))
        return (inner | edge) if p in (0, 2) else inner

    def start_own_piece(p):
        @pl.when(hi + 1 < outer)
        def _():
            hop(col, p, 0).start()

        @pl.when(hi > 0)
        def _():
            hop(col, p, 1).start()

        hop(col, p, 2).start()

    for k in range(1, n_col):
        p_copy(k).start()
    assemble(0)
    start_own_piece(0)
    for k in [*range(2, n_row), 1]:
        pick(k)
        x_copy(k).start()

    x_copy(1).wait_recv()
    assemble(1)
    start_own_piece(1)

    mine = okc & (dc == colf)
    coded = jnp.broadcast_to(jnp.where(okc, dc * 8.0 + rank_slot + 1.0, 0.0), (W, LANE)).astype(BF)

    def atom_of(t):
        return jnp.where(t < s_.cols, whole_part(t, NBF), -1.0e4)

    atom_c, atom_r = atom_of(fiota((blk, 1), 0)), atom_of(fiota((1, blk), 1))
    within = fiota((blk, 1), 0) - NBF * atom_c
    my_tile = pl.multiple_of(col * slot // LANE * LANE, LANE)
    my_lane = (col * slot % LANE).astype(F32)
    pull_place = expand(mine, NBF * vc, bc * LANE + my_lane + NBF * rank_slot, blk)

    def chunk_tables(c, _):
        code = mm(jnp.where(nar - (c * ac).astype(F32) == atom_c, 1.0, 0.0).astype(BF), coded) - 1.0
        far = jnp.floor(code * 0.125)
        at = far * slot + NBF * (code - 8.0 * far) + within
        pos[c] = jnp.where(code < 0.0, -1.0, at)
        rows = pl.ds(pl.multiple_of(c * LANE, LANE), LANE)
        pull[rows, :] = onehot(LANE, pull_place - (c * LANE).astype(F32))
        return 0

    def masks_and_tables():
        er_at = fiota((1, LANE), 1)
        er_d = whole_part(er_at, ac)
        er_w = (rowf * ratio + er_d) * av + er_at - er_d * ac
        first = jnp.sum(jnp.where((wc == er_w) & (er_at < ar), NBF * rank_all + 1.0e6, 0.0), axis=0, keepdims=True) - 1.0e6
        u = fiota((live, LANE), 0) - first
        er = jnp.where((u >= 0.0) & (u < NBF), 1.0, 0.0).astype(BF)

        for k in range(1, n_col):
            src = (col + k) % n_col
            pltpu.make_async_copy(pt_all.at[src], pt_all.at[src], p_recv.at[src]).wait()
        mr[...] = mm_nt(er, pt_all[...].reshape(W, LANE)).astype(BF)
        lax.fori_loop(0, n_col, chunk_tables, 0)


    def process(c, g):
        i0, i1 = s_.spans[g]
        n = i1 - i0
        hit = jnp.where(nac - c.astype(F32) * ac == atom_r, 1.0, 0.0).astype(BF)
        keep = mm(mr[i0:i1, :], hit)
        part = jnp.where(keep > 0.5, panel[c, i0:i1, :].astype(F32), 0.0)
        tot[...] += jnp.sum((part * part).reshape(n // 8, 8, blk), axis=0)
        at = pos[c]
        lane = fiota((blk, LANE), 1)
        to_slot = jnp.concatenate(
            [jnp.where(lane + float(q) == at, 1.0, 0.0).astype(BF) for q in range(0, slots, LANE)], axis=1
        )
        left[i0:i1, pl.ds(pl.multiple_of(c * slots, slots), slots)] = mm(part.astype(BF), to_slot).astype(BF)

    def arrived(c, p):
        pltpu.make_async_copy(piece(c, p), piece(c, p), g_recv.at[c, p]).wait()

    def forward(d, g):
        for p in s_.groups[g]:
            for way in range(2):
                src = hi - d if way == 0 else hi + d

                @pl.when((src >= 0) & (src < outer))
                def _():
                    c = src * 2 + lo
                    arrived(c, p)

                    @pl.when(hi + 1 < outer if way == 0 else hi > 0)
                    def _():
                        hop(c, p, way).start()

                    @pl.when(jnp.logical_not(by_line(hi, src, p)))
                    def _():
                        hop(c, p, 2).start()

            @pl.when(d == 1)
            def _():
                c = hi * 2 + 1 - lo
                arrived(c, p)

                @pl.when((hi + 1 < outer) & by_line(hi + 1, hi, p))
                def _():
                    hop(c, p, 0).start()

                @pl.when((hi > 0) & by_line(hi - 1, hi, p))
                def _():
                    hop(c, p, 1).start()

    def work(e, g):
        def candidate(k, _):
            kind, way = k // 2, k % 2
            dist = e - 1 - kind
            src = hi + (1 - 2 * way) * dist
            ok = (dist >= 0) & (dist < outer) & (src >= 0) & (src < outer) & ((dist > 0) | (way == 0))

            @pl.when(ok)
            def _():
                c = src * 2 + jnp.where(kind == 0, lo, 1 - lo)

                @pl.when((kind == 1) & (dist > 0))
                def _():
                    for p in s_.groups[g]:
                        arrived(c, p)

                process(c, g)

            return 0

        lax.fori_loop(0, 4, candidate, 0)

    def gather(g, between):
        def step(d, _):
            forward(d, g)
            for at, extra in between.items():
                pl.when(d == at)(extra)
            if g > 0:

                @pl.when(d <= 2)
                def _():
                    work(outer - 1 + d, g - 1)

                @pl.when(d == 2)
                def _():
                    right_share(g - 1)

            work(d, g)
            return 0

        lax.fori_loop(1, outer, step, 0)

    def part_of(r, ix):
        if ix < n_group:
            i0, i1 = s_.spans[ix]
            return rt.at[r, pl.ds(i0, i1 - i0), :]
        return (sta, stb)[ix - n_group].at[r, pl.ds(0, live), :]

    def share(ix):
        def send(r, to, sem):
            return pltpu.make_async_remote_copy(
                src_ref=part_of(r, ix), dst_ref=part_of(r, ix), send_sem=sem, recv_sem=r_recv.at[ix, r],
                device_id={"row": to, "col": col}, device_id_type=MESH,
            )

        return (
            [send(row, (x + k) % nx * 2 + core, r_send.at[ix, k]) for k in range(1, nx)]
            + [send(row, peer, r_send.at[ix, 0])],
            [send((x + k) % nx * 2 + core, peer, f_send.at[ix, k]) for k in range(1, nx)],
        )

    def start_share(ix):
        for cp in share(ix)[0]:
            cp.start()

    def got(ix, r):
        pltpu.make_async_copy(part_of(r, ix), part_of(r, ix), r_recv.at[ix, r]).wait()

    def relay(ix):
        onward = share(ix)[1]
        for k in range(1, nx):
            got(ix, (x + k) % nx * 2 + core)
            onward[k - 1].start()

    def finish(ix):
        for k in range(nx):
            got(ix, (x + k) % nx * 2 + 1 - core)

    def right_share(g):
        i0, i1 = s_.spans[g]
        mine_first = jnp.concatenate([left[i0:i1, pl.ds(c * slots + my_tile, LANE)] for c in range(n_col)], axis=1)
        rt[row, i0:i1, :] = mm(mine_first, pull[...]).astype(BF)
        start_share(g)

    def later_rows():
        for k in range(2, n_row):
            x_copy(k).wait_recv()
        for p in range(2, n_piece):
            assemble(p)
            start_own_piece(p)

    def row_places(r):
        ws = slice(r * ratio * av, (r + 1) * ratio * av)
        at = (dc[ws] - float(r * ratio)) * slots + bc[ws] * slot + NBF * rank_slot[ws]
        return expand(okc[ws], NBF * rank_all[ws], at, wide)

    def row_slots(r, a, b):
        return xm[r, :, a:b] if s_.stored else onehot(ratio * slots, xm[r, 0:1, a:b])

    def row_blocks(visit):
        if s_.stored:
            for r in range(n_row):
                visit(r)
        else:
            lax.fori_loop(0, n_row, lambda r, _: (visit(r), 0)[1], 0)

    def tables():
        for r in range(n_row):
            at = row_places(r)
            xm[r] = onehot(ratio * slots, at) if s_.stored else jnp.broadcast_to(at, (8, wide))
        my_new = NBF * ((dc - rowf * ratio) * ac + vc)
        fm[...] = onehot(s_.rows, expand(to_me, NBF * rank_all, my_new, wide))
        t = fiota((W, blk), 1) - NBF * vc
        kq[...] = mm(mr[...], jnp.where((t >= 0.0) & (t < NBF) & mine, 1.0, 0.0).astype(BF)).astype(BF)

    gather(0, {1: masks_and_tables, 2: later_rows})
    gather(1, {1: tables})
    gather(2, {1: lambda: relay(0)})
    last = n_group - 1

    def tail(e, _):
        work(e, last)
        return 0

    lax.fori_loop(outer, outer + 2, tail, 0)
    right_share(last)
    relay(1)

    def t_copy(k):
        return pltpu.make_async_remote_copy(
            src_ref=tot_all.at[row], dst_ref=tot_all.at[row], send_sem=t_send.at[k], recv_sem=t_recv.at[row],
            device_id={"row": (row + k) % n_row, "col": col}, device_id_type=MESH,
        )

    part_sum = tot[:, 0:LANE]
    for q in range(1, blk // LANE):
        part_sum += tot[:, q * LANE : (q + 1) * LANE]
    tot_all[row] = part_sum
    for k in range(1, n_row):
        t_copy(k).start()
    finish(0)
    finish(1)
    early = s_.spans[2][0] // LANE * LANE

    def spread(r, rows, j0, width, add):
        for q in range(n_col * ratio):
            at = pl.ds(r * ratio * slot + q % n_col * slots + q // n_col * slot, slot)
            if not s_.stored:
                at = pl.ds(pl.multiple_of(at.start, slot), slot)
            part = rows[q * slot : (q + 1) * slot].astype(BF)
            if add:
                rx[at, j0 : j0 + width] += part
            else:
                rx[at, j0 : j0 + width] = part

    row_blocks(lambda r: spread(r, mm(row_slots(r, 0, early), rt[r, 0:early, :]), 0, blk, False))
    relay(2)
    finish(2)
    row_blocks(lambda r: spread(r, mm(row_slots(r, early, wide), rt[r, early:, :]), 0, blk, True))
    for k in range(1, n_row):
        src = (row + k) % n_row
        pltpu.make_async_copy(tot_all.at[src], tot_all.at[src], t_recv.at[src]).wait()
    total = jnp.sum(jnp.sum(tot_all[...], axis=0), axis=(0, 1), keepdims=True)
    scale = lax.rsqrt(total / order)

    half = live // 2

    def product(i0, j0, width):
        depth = min(n_col * slots, 4096)
        if depth == n_col * slots:
            return mm(left[i0 : i0 + half, :], rx[:, j0 : j0 + width])

        def more(q, acc):
            k = pl.ds(pl.multiple_of(q * slots, slots), slots)
            return acc + mm(left[i0 : i0 + half, k], rx[k, j0 : j0 + width])

        return lax.fori_loop(0, n_col, more, jnp.zeros((half, width), F32))

    for q, (j0, width) in enumerate(s_.joff):
        st = (sta, stb)[q]
        for i0 in (0, half):
            square = product(i0, j0, width) * scale * scale
            keep = kq[i0 : i0 + half, j0 : j0 + width].astype(F32)
            st[row, i0 : i0 + half, :] = jnp.where(keep > 0.5, square, 0.0).astype(BF)
        start_share(n_group + q)

    start = (rt[row].astype(F32) * scale).astype(BF)
    moved = 1.5 * mm(fm[...], start)
    out_ref[...] = moved[:, 0 : s_.cols]

    for k in range(1, n_row):
        x_copy(k).wait_send()
        t_copy(k).wait_send()
    for k in range(1, n_col):
        p_copy(k).wait_send()
    for p in range(n_piece):

        def sent(q, _):
            c = q * 2 + lo

            @pl.when((q <= hi) & (hi + 1 < outer))
            def _():
                hop(c, p, 0).wait_send()

            @pl.when((q >= hi) & (hi > 0))
            def _():
                hop(c, p, 1).wait_send()

            @pl.when((q == hi) | jnp.logical_not(by_line(hi, q, p)))
            def _():
                hop(c, p, 2).wait_send()

            return 0

        lax.fori_loop(0, outer, sent, 0)
        c_other = hi * 2 + 1 - lo

        @pl.when((hi + 1 < outer) & by_line(hi + 1, hi, p))
        def _():
            hop(c_other, p, 0).wait_send()

        @pl.when((hi > 0) & by_line(hi - 1, hi, p))
        def _():
            hop(c_other, p, 1).wait_send()

    def sent_share(ix):
        first, onward = share(ix)
        for cp in first + onward:
            cp.wait_send()

    for ix in range(n_group):
        sent_share(ix)

    cac[live:, :] = jnp.zeros((wide - live, blk), BF)
    for q, (j0, width) in enumerate(s_.joff):
        st = (sta, stb)[q]
        if q == 0:
            relay(n_group)
        finish(n_group + q)
        row_blocks(lambda r: spread(r, mm(row_slots(r, 0, wide), st[r]), j0, width, False))
        for i0 in (0, half):
            cube = product(i0, j0, width) * scale
            keep = kq[i0 : i0 + half, j0 : j0 + width].astype(F32)
            cac[i0 : i0 + half, j0 : j0 + width] = jnp.where(keep > 0.5, cube, 0.0).astype(BF)
        if q == 0:
            relay(n_group + 1)
        done = mm(fm[...], cac[:, j0 : j0 + width])
        end = min(j0 + width, s_.cols)
        out_ref[:, j0:end] -= 0.5 * done[:, 0 : end - j0]

    for q in range(2):
        sent_share(n_group + q)


def on_device(hamiltonian, new_atom, pattern):
    rows, cols = hamiltonian.shape
    n_row, n_col = lax.axis_size("row"), lax.axis_size("col")
    ar, ac = pattern.shape
    s = Plan(n_row, n_col, rows, cols, ar, ac)
    vm = pl.BlockSpec(memory_space=pltpu.VMEM)
    dma = pltpu.SemaphoreType.DMA
    n_piece = len(s.sizes)
    n_group = len(s.groups)
    slots = n_col * s.slot
    buffers = [
        pltpu.VMEM((s.wide, s.blk), BF),
        pltpu.VMEM((n_row - 1, s.sl, s.blk), BF),
        pltpu.VMEM((n_row - 1, s.slp, s.blk), BF),
        pltpu.VMEM((s.av, LANE), F32),
        pltpu.VMEM((n_col, s.av, LANE), BF),
        pltpu.VMEM((s.live, s.w), BF),
        pltpu.VMEM((s.live, s.blk), BF),
        pltpu.VMEM((n_col, s.live, s.blk), BF),
        pltpu.VMEM((s.live, n_col * slots), BF),
        pltpu.VMEM((n_col, s.blk, LANE), F32),
        pltpu.VMEM((n_col * LANE, s.blk), BF),
        pltpu.VMEM((n_row, s.wide, s.blk), BF),
        pltpu.VMEM((n_col * slots, s.blk), BF),
        pltpu.VMEM((n_row, s.ratio * slots, s.wide) if s.stored else (n_row, 8, s.wide), BF if s.stored else F32),
        pltpu.VMEM((rows, s.wide), BF),
        pltpu.VMEM((n_row, s.wide, s.joff[0][1]), BF),
        pltpu.VMEM((n_row, s.wide, s.joff[1][1]), BF),
        pltpu.VMEM((s.wide, s.blk), BF),
        pltpu.VMEM((8, s.blk), F32),
        pltpu.VMEM((n_row, 8, LANE), F32),
    ]
    held = sum(int(np.prod(b.shape)) * np.dtype(b.dtype).itemsize for b in buffers)
    return pl.pallas_call(
        functools.partial(kernel, s, float(rows * n_row)),
        out_shape=jax.ShapeDtypeStruct((rows, cols), F32),
        in_specs=[vm, vm, vm],
        out_specs=vm,
        scratch_shapes=[
            *buffers,
            dma((n_row,)),
            dma((n_row,)),
            dma((n_col,)),
            dma((n_col,)),
            dma((n_row,)),
            dma((n_row,)),
            dma((3, n_col, n_piece)),
            dma((n_col, n_piece)),
            dma((n_group + 2, n_row)),
            dma((n_group + 2, n_row)),
            dma((n_group + 2, n_row)),
        ],
        compiler_params=pltpu.CompilerParams(
            collective_id=0, has_side_effects=True, vmem_limit_bytes=min(held + held // 8 + 7 * 1024 * 1024, 62 * 1024 * 1024)
        ),
    )(hamiltonian, new_atom.reshape(1, -1), pattern.T)


def solution(mesh):
    in_specs = (P("row", "col"), P(), P("row", "col"))
    out_specs = P("row", "col")
    return jax.shard_map(
        on_device, mesh=mesh, in_specs=in_specs, out_specs=out_specs, check_vma=False
    )
```

```python
import functools

import jax
import jax.numpy as jnp
import numpy as np
from jax import lax
from jax.experimental import pallas as pl
from jax.experimental.pallas import tpu as pltpu
from jax.sharding import PartitionSpec as P

NBF = 13
LANE = 128
BF = jnp.bfloat16
F32 = jnp.float32
I32 = jnp.int32
MESH = pl.DeviceIdType.MESH
FAR = -1.0e6


def up(n, k):
    return -(-n // k) * k


def mm(a, b):
    return jnp.dot(a, b, preferred_element_type=F32)


def mm_nt(a, b):
    return lax.dot_general(a, b, (((1,), (1,)), ((), ())), preferred_element_type=F32)


def iota(shape, axis):
    return lax.broadcasted_iota(I32, shape, axis)


def fiota(shape, axis):
    return iota(shape, axis).astype(F32)


def whole_part(x, n):
    return jnp.floor((x + 0.5) * (1.0 / n))


def expand(sel, lo, start, size):
    u = fiota((lo.shape[0], size), 1) - lo
    hit = sel & (u >= 0.0) & (u < NBF)
    return jnp.sum(jnp.where(hit, u + (start + 1.0), 0.0), axis=0, keepdims=True) - 1.0


def onehot(rows, places, offset=0):
    i = fiota((rows, places.shape[1]), 0) + float(offset)
    return jnp.where(i == places, 1.0, 0.0).astype(BF)


class Plan:
    def __init__(self, n_row, n_col, rows, cols, ar, ac):
        self.n_row, self.n_col, self.rows, self.cols, self.ar, self.ac = n_row, n_col, rows, cols, ar, ac
        self.ratio = n_col // n_row
        self.nx = n_row // 2
        self.outer = n_col // 2
        self.av = up(ac, 16)
        self.w = n_col * self.av
        self.blk = up(cols, LANE)
        self.live = up(rows, 16)
        self.wide = up(rows, LANE)
        count = np.bincount((1 + np.arange(ac)) % n_col, minlength=n_col)
        self.slot = up(int(count.max()) * NBF, 16)
        r = self.ratio
        pair = [
            sum(int(count[(r * k + g - b) % n_col]) for b in range(r) for g in range(r)) for k in range(n_row)
        ]
        self.sl = up(max(pair) * NBF, 16)
        self.slp = up(self.sl, LANE)
        own = pair[0] * NBF // 16 * 16
        chip = (pair[0] + min(pair[1], pair[n_row - 1])) * NBF // 16 * 16
        rest = self.live - chip
        last = up(rest // 3, 16)
        mid = up((rest - last) // 2, 16)
        ends = [0, own, chip, chip + mid, self.live - last, self.live]
        self.starts, self.sizes = ends[:-1], [b - a for a, b in zip(ends, ends[1:])]
        self.groups = [[0, 1], [2, 3], [4]]
        self.spans = [(ends[g[0]], ends[g[-1] + 1]) for g in self.groups]
        self.stored = n_row * self.ratio * n_col * self.slot * self.wide * 2 <= 8 * 1024 * 1024
        self.joff = [(0, self.blk - LANE), (self.blk - LANE, LANE)]


def kernel(
    s_, order, h_ref, na_ref, pat_ref, out_ref,
    hp, xs, rin, pp, pt_all, mr, kq, panel, left, pos, pull, rt, rx, xm, fm, sta, stb, cac, tot, tot_all,
    x_send, x_recv, p_send, p_recv, t_send, t_recv, g_send, g_recv, r_send, r_recv, f_send,
):
    n_row, n_col, ratio, nx, outer = s_.n_row, s_.n_col, s_.ratio, s_.nx, s_.outer
    ac, ar, av, W, blk, live, wide = s_.ac, s_.ar, s_.av, s_.w, s_.blk, s_.live, s_.wide
    slot, sl, slp = s_.slot, s_.sl, s_.slp
    row = lax.axis_index("row")
    col = lax.axis_index("col")
    hi, lo = col // 2, col % 2
    x, core = row // 2, row % 2
    peer = x * 2 + 1 - core
    n_piece = len(s_.sizes)
    n_group = len(s_.groups)
    slots = n_col * slot

    barrier = pltpu.get_barrier_semaphore()
    for k in range(1, n_row):
        pl.semaphore_signal(barrier, inc=1, device_id={"row": (row + k) % n_row, "col": col}, device_id_type=MESH)
    for k in range(1, n_col):
        pl.semaphore_signal(barrier, inc=1, device_id={"row": row, "col": (col + k) % n_col}, device_id_type=MESH)

    rowf, colf, xf, coref, peerf = [i.astype(F32) for i in (row, col, x, core, peer)]

    def places(w):
        d = whole_part(w, av)
        v = w - d * av
        return d, v, v < ac

    def source(na, d):
        b = whole_part(na, ac)
        src = whole_part(b, ratio)
        home = whole_part(d, ratio)
        far = jnp.where(whole_part(src, 2) == whole_part(home, 2), 1.0, 2.0)
        return b, src, home, jnp.where(src == home, 0.0, far)

    wc, wr = fiota((W, 1), 0), fiota((1, W), 1)
    dc, vc, okc = places(wc)
    dr, vr, okr = places(wr)
    atoms = na_ref[...].astype(F32)
    here = (fiota((W, atoms.shape[1]), 1) == dc * ac + vc) & okc
    nac = jnp.where(okc, jnp.sum(jnp.where(here, atoms, 0.0), axis=1, keepdims=True), -1.0e5)
    nar = jnp.sum(jnp.where(fiota((W, W), 0) == wr, nac, 0.0), axis=0, keepdims=True)
    bc, srcc, homec, grpc = source(nac, dc)
    br, srcr, homer, grpr = source(nar, dr)
    before = wr < wc

    def rank(hit):
        return jnp.sum(jnp.where(hit & okr, 1.0, 0.0), axis=1, keepdims=True)

    rank_slot = rank((dr == dc) & (br == bc) & before)
    rank_pair = rank((homer == homec) & (srcr == srcc) & before)
    rank_all = rank((homer == homec) & ((grpr < grpc) | ((grpr == grpc) & before)))
    old_at = NBF * (nac - srcc * ar)
    kx = whole_part(homec, 2) - xf
    kx = jnp.where(kx < 0.0, kx + nx, kx)
    kc = homec - 2.0 * whole_part(homec, 2)
    kc = jnp.where(kc == coref, 0.0, 1.0)
    from_me = okc & (srcc == rowf)
    to_me = okc & (homec == rowf)
    out_place = expand(from_me, old_at, (2.0 * kx + kc) * slp + NBF * rank_pair, wide)
    own_place = expand(from_me & to_me, old_at, NBF * rank_all, wide)

    def other(sign, k):
        return ((x + sign * (k // 2) + nx) % nx) * 2 + (core + k % 2) % 2

    in_place = {
        k: expand(to_me & (srcc == other(-1, k).astype(F32)), NBF * rank_pair, NBF * rank_all, slp)
        for k in range(1, n_row)
    }

    pp[...] = jnp.zeros_like(pp)
    pp[0:ac, 0:ar] = pat_ref[...].astype(F32)
    pt_all[col] = pp[...].astype(BF)
    hp[...] = jnp.zeros_like(hp)
    rin[:, sl:, :] = jnp.zeros((n_row - 1, slp - sl, blk), BF)
    rt[:, live:, :] = jnp.zeros((n_row, wide - live, blk), BF)
    sta[:, live:, :] = jnp.zeros((n_row, wide - live, sta.shape[2]), BF)
    stb[:, live:, :] = jnp.zeros((n_row, wide - live, stb.shape[2]), BF)
    tot[...] = jnp.zeros_like(tot)
    hp[0 : s_.rows, 0 : s_.cols] = h_ref[...]

    def pick(k):
        xs[k - 1] = mm(onehot(sl, out_place, k * slp), hp[...]).astype(BF)

    def piece(c, p):
        return panel.at[c, pl.ds(s_.starts[p], s_.sizes[p]), :]

    def assemble(p):
        i0, n = s_.starts[p], s_.sizes[p]
        part = None
        if p < 2:
            part = mm(onehot(n, own_place, i0), hp[...])
        for k in range(1, n_row):
            if p >= (1 if k == 1 else 2):
                more = mm(onehot(n, in_place[k], i0), rin[k - 1])
                part = more if part is None else part + more
        panel[col, i0 : i0 + n, :] = part.astype(BF)

    assemble(0)
    pl.semaphore_wait(barrier, n_row + n_col - 2)

    def x_copy(k):
        return pltpu.make_async_remote_copy(
            src_ref=xs.at[k - 1], dst_ref=rin.at[k - 1, pl.ds(0, sl), :],
            send_sem=x_send.at[k], recv_sem=x_recv.at[k],
            device_id={"row": other(1, k), "col": col}, device_id_type=MESH,
        )

    def p_copy(k):
        return pltpu.make_async_remote_copy(
            src_ref=pt_all.at[col], dst_ref=pt_all.at[col], send_sem=p_send.at[k], recv_sem=p_recv.at[col],
            device_id={"row": row, "col": (col + k) % n_col}, device_id_type=MESH,
        )

    def hop(c, p, way):
        to = [col + 2, col - 2, hi * 2 + 1 - lo][way]
        return pltpu.make_async_remote_copy(
            src_ref=piece(c, p), dst_ref=piece(c, p),
            send_sem=g_send.at[way, c, p], recv_sem=g_recv.at[c, p],
            device_id={"row": row, "col": to}, device_id_type=MESH,
        )

    def by_line(at, src, p):
        inner = ((at == 1) & (src == 0)) | ((at == outer - 2) & (src == outer - 1))
        edge = ((at == outer - 1) & (src == outer - 2)) | ((at == 0) & (src == 1))
        return (inner | edge) if p in (0, 2) else inner

    def start_own_piece(p):
        @pl.when(hi + 1 < outer)
        def _():
            hop(col, p, 0).start()

        @pl.when(hi > 0)
        def _():
            hop(col, p, 1).start()

        hop(col, p, 2).start()

    start_own_piece(0)
    for k in range(1, n_col):
        p_copy(k).start()
    for k in [*range(2, n_row), 1]:
        pick(k)
        x_copy(k).start()

    x_copy(1).wait_recv()
    assemble(1)
    start_own_piece(1)

    mine = okc & (dc == colf)
    coded = jnp.broadcast_to(jnp.where(okc, dc * 8.0 + rank_slot + 1.0, 0.0), (W, LANE)).astype(BF)

    def atom_of(t):
        return jnp.where(t < s_.cols, whole_part(t, NBF), -1.0e4)

    atom_c, atom_r = atom_of(fiota((blk, 1), 0)), atom_of(fiota((1, blk), 1))
    within = fiota((blk, 1), 0) - NBF * atom_c
    my_tile = pl.multiple_of(col * slot // LANE * LANE, LANE)
    my_lane = (col * slot % LANE).astype(F32)
    pull_place = expand(mine, NBF * vc, bc * LANE + my_lane + NBF * rank_slot, blk)

    def chunk_tables(c, _):
        code = mm(jnp.where(nar - (c * ac).astype(F32) == atom_c, 1.0, 0.0).astype(BF), coded) - 1.0
        far = jnp.floor(code * 0.125)
        at = far * slot + NBF * (code - 8.0 * far) + within
        pos[c] = jnp.where(code < 0.0, -1.0, at)
        rows = pl.ds(pl.multiple_of(c * LANE, LANE), LANE)
        pull[rows, :] = onehot(LANE, pull_place - (c * LANE).astype(F32))
        return 0

    def masks_and_tables():
        er_at = fiota((1, LANE), 1)
        er_d = whole_part(er_at, ac)
        er_w = (rowf * ratio + er_d) * av + er_at - er_d * ac
        first = jnp.sum(jnp.where((wc == er_w) & (er_at < ar), NBF * rank_all + 1.0e6, 0.0), axis=0, keepdims=True) - 1.0e6
        u = fiota((live, LANE), 0) - first
        er = jnp.where((u >= 0.0) & (u < NBF), 1.0, 0.0).astype(BF)

        for k in range(1, n_col):
            src = (col + k) % n_col
            pltpu.make_async_copy(pt_all.at[src], pt_all.at[src], p_recv.at[src]).wait()
        mr[...] = mm_nt(er, pt_all[...].reshape(W, LANE)).astype(BF)
        lax.fori_loop(0, n_col, chunk_tables, 0)


    def process(c, g):
        i0, i1 = s_.spans[g]
        n = i1 - i0
        hit = jnp.where(nac - c.astype(F32) * ac == atom_r, 1.0, 0.0).astype(BF)
        keep = mm(mr[i0:i1, :], hit)
        part = jnp.where(keep > 0.5, panel[c, i0:i1, :].astype(F32), 0.0)
        tot[...] += jnp.sum((part * part).reshape(n // 8, 8, blk), axis=0)
        at = pos[c]
        lane = fiota((blk, LANE), 1)
        to_slot = jnp.concatenate(
            [jnp.where(lane + float(q) == at, 1.0, 0.0).astype(BF) for q in range(0, slots, LANE)], axis=1
        )
        left[i0:i1, pl.ds(pl.multiple_of(c * slots, slots), slots)] = mm(part.astype(BF), to_slot).astype(BF)

    def arrived(c, p):
        pltpu.make_async_copy(piece(c, p), piece(c, p), g_recv.at[c, p]).wait()

    def forward(d, g):
        for p in s_.groups[g]:
            for way in range(2):
                src = hi - d if way == 0 else hi + d

                @pl.when((src >= 0) & (src < outer))
                def _():
                    c = src * 2 + lo
                    arrived(c, p)

                    @pl.when(hi + 1 < outer if way == 0 else hi > 0)
                    def _():
                        hop(c, p, way).start()

                    @pl.when(jnp.logical_not(by_line(hi, src, p)))
                    def _():
                        hop(c, p, 2).start()

            @pl.when(d == 1)
            def _():
                c = hi * 2 + 1 - lo
                arrived(c, p)

                @pl.when((hi + 1 < outer) & by_line(hi + 1, hi, p))
                def _():
                    hop(c, p, 0).start()

                @pl.when((hi > 0) & by_line(hi - 1, hi, p))
                def _():
                    hop(c, p, 1).start()

    def work(e, g):
        def candidate(k, _):
            kind, way = k // 2, k % 2
            dist = e - 1 - kind
            src = hi + (1 - 2 * way) * dist
            ok = (dist >= 0) & (dist < outer) & (src >= 0) & (src < outer) & ((dist > 0) | (way == 0))

            @pl.when(ok)
            def _():
                c = src * 2 + jnp.where(kind == 0, lo, 1 - lo)

                @pl.when((kind == 1) & (dist > 0))
                def _():
                    for p in s_.groups[g]:
                        arrived(c, p)

                process(c, g)

            return 0

        lax.fori_loop(0, 4, candidate, 0)

    def gather(g, between):
        def step(d, _):
            forward(d, g)
            for at, extra in between.items():
                pl.when(d == at)(extra)
            if g > 0:

                @pl.when(d <= 2)
                def _():
                    work(outer - 1 + d, g - 1)

                @pl.when(d == 2)
                def _():
                    right_share(g - 1)

            work(d, g)
            return 0

        lax.fori_loop(1, outer, step, 0)

    def part_of(r, ix):
        if ix < n_group:
            i0, i1 = s_.spans[ix]
            return rt.at[r, pl.ds(i0, i1 - i0), :]
        return (sta, stb)[ix - n_group].at[r, pl.ds(0, live), :]

    def share(ix):
        def send(r, to, sem):
            return pltpu.make_async_remote_copy(
                src_ref=part_of(r, ix), dst_ref=part_of(r, ix), send_sem=sem, recv_sem=r_recv.at[ix, r],
                device_id={"row": to, "col": col}, device_id_type=MESH,
            )

        return (
            [send(row, (x + k) % nx * 2 + core, r_send.at[ix, k]) for k in range(1, nx)]
            + [send(row, peer, r_send.at[ix, 0])],
            [send((x + k) % nx * 2 + core, peer, f_send.at[ix, k]) for k in range(1, nx)],
        )

    def start_share(ix):
        for cp in share(ix)[0]:
            cp.start()

    def got(ix, r):
        pltpu.make_async_copy(part_of(r, ix), part_of(r, ix), r_recv.at[ix, r]).wait()

    def relay(ix):
        onward = share(ix)[1]
        for k in range(1, nx):
            got(ix, (x + k) % nx * 2 + core)
            onward[k - 1].start()

    def finish(ix):
        for k in range(nx):
            got(ix, (x + k) % nx * 2 + 1 - core)

    def right_share(g):
        i0, i1 = s_.spans[g]
        mine_first = jnp.concatenate([left[i0:i1, pl.ds(c * slots + my_tile, LANE)] for c in range(n_col)], axis=1)
        rt[row, i0:i1, :] = mm(mine_first, pull[...]).astype(BF)
        start_share(g)

    def later_rows():
        for k in range(2, n_row):
            x_copy(k).wait_recv()
        for p in range(2, n_piece):
            assemble(p)
            start_own_piece(p)

    def row_places(r):
        ws = slice(r * ratio * av, (r + 1) * ratio * av)
        at = (dc[ws] - float(r * ratio)) * slots + bc[ws] * slot + NBF * rank_slot[ws]
        return expand(okc[ws], NBF * rank_all[ws], at, wide)

    def row_slots(r, a, b):
        return xm[r, :, a:b] if s_.stored else onehot(ratio * slots, xm[r, 0:1, a:b])

    def row_blocks(visit):
        if s_.stored:
            for r in range(n_row):
                visit(r)
        else:
            lax.fori_loop(0, n_row, lambda r, _: (visit(r), 0)[1], 0)

    def tables():
        for r in range(n_row):
            at = row_places(r)
            xm[r] = onehot(ratio * slots, at) if s_.stored else jnp.broadcast_to(at, (8, wide))
        my_new = NBF * ((dc - rowf * ratio) * ac + vc)
        fm[...] = onehot(s_.rows, expand(to_me, NBF * rank_all, my_new, wide))
        t = fiota((W, blk), 1) - NBF * vc
        kq[...] = mm(mr[...], jnp.where((t >= 0.0) & (t < NBF) & mine, 1.0, 0.0).astype(BF)).astype(BF)

    gather(0, {1: masks_and_tables, 2: later_rows})
    gather(1, {1: tables})
    gather(2, {1: lambda: relay(0)})
    last = n_group - 1

    def tail(e, _):
        work(e, last)
        return 0

    lax.fori_loop(outer, outer + 2, tail, 0)
    right_share(last)
    relay(1)

    def t_copy(k):
        return pltpu.make_async_remote_copy(
            src_ref=tot_all.at[row], dst_ref=tot_all.at[row], send_sem=t_send.at[k], recv_sem=t_recv.at[row],
            device_id={"row": (row + k) % n_row, "col": col}, device_id_type=MESH,
        )

    part_sum = tot[:, 0:LANE]
    for q in range(1, blk // LANE):
        part_sum += tot[:, q * LANE : (q + 1) * LANE]
    tot_all[row] = part_sum
    for k in range(1, n_row):
        t_copy(k).start()
    finish(0)
    finish(1)
    early = s_.spans[2][0] // LANE * LANE

    def spread(r, rows, j0, width, add):
        for q in range(n_col * ratio):
            at = pl.ds(r * ratio * slot + q % n_col * slots + q // n_col * slot, slot)
            if not s_.stored:
                at = pl.ds(pl.multiple_of(at.start, slot), slot)
            part = rows[q * slot : (q + 1) * slot].astype(BF)
            if add:
                rx[at, j0 : j0 + width] += part
            else:
                rx[at, j0 : j0 + width] = part

    row_blocks(lambda r: spread(r, mm(row_slots(r, 0, early), rt[r, 0:early, :]), 0, blk, False))
    relay(2)
    finish(2)
    row_blocks(lambda r: spread(r, mm(row_slots(r, early, wide), rt[r, early:, :]), 0, blk, True))
    for k in range(1, n_row):
        src = (row + k) % n_row
        pltpu.make_async_copy(tot_all.at[src], tot_all.at[src], t_recv.at[src]).wait()
    total = jnp.sum(jnp.sum(tot_all[...], axis=0), axis=(0, 1), keepdims=True)
    scale = lax.rsqrt(total / order)

    half = live // 2

    def product(i0, j0, width):
        depth = min(n_col * slots, 4096)
        if depth == n_col * slots:
            return mm(left[i0 : i0 + half, :], rx[:, j0 : j0 + width])

        def more(q, acc):
            k = pl.ds(pl.multiple_of(q * slots, slots), slots)
            return acc + mm(left[i0 : i0 + half, k], rx[k, j0 : j0 + width])

        return lax.fori_loop(0, n_col, more, jnp.zeros((half, width), F32))

    for q, (j0, width) in enumerate(s_.joff):
        st = (sta, stb)[q]
        for i0 in (0, half):
            square = product(i0, j0, width) * scale * scale
            keep = kq[i0 : i0 + half, j0 : j0 + width].astype(F32)
            st[row, i0 : i0 + half, :] = jnp.where(keep > 0.5, square, 0.0).astype(BF)
        start_share(n_group + q)

    start = (rt[row].astype(F32) * scale).astype(BF)
    moved = 1.5 * mm(fm[...], start)
    out_ref[...] = moved[:, 0 : s_.cols]

    for k in range(1, n_row):
        x_copy(k).wait_send()
        t_copy(k).wait_send()
    for k in range(1, n_col):
        p_copy(k).wait_send()
    for p in range(n_piece):

        def sent(q, _):
            c = q * 2 + lo

            @pl.when((q <= hi) & (hi + 1 < outer))
            def _():
                hop(c, p, 0).wait_send()

            @pl.when((q >= hi) & (hi > 0))
            def _():
                hop(c, p, 1).wait_send()

            @pl.when((q == hi) | jnp.logical_not(by_line(hi, q, p)))
            def _():
                hop(c, p, 2).wait_send()

            return 0

        lax.fori_loop(0, outer, sent, 0)
        c_other = hi * 2 + 1 - lo

        @pl.when((hi + 1 < outer) & by_line(hi + 1, hi, p))
        def _():
            hop(c_other, p, 0).wait_send()

        @pl.when((hi > 0) & by_line(hi - 1, hi, p))
        def _():
            hop(c_other, p, 1).wait_send()

    def sent_share(ix):
        first, onward = share(ix)
        for cp in first + onward:
            cp.wait_send()

    for ix in range(n_group):
        sent_share(ix)

    cac[live:, :] = jnp.zeros((wide - live, blk), BF)
    for q, (j0, width) in enumerate(s_.joff):
        st = (sta, stb)[q]
        if q == 0:
            relay(n_group)
        finish(n_group + q)
        row_blocks(lambda r: spread(r, mm(row_slots(r, 0, wide), st[r]), j0, width, False))
        for i0 in (0, half):
            cube = product(i0, j0, width) * scale
            keep = kq[i0 : i0 + half, j0 : j0 + width].astype(F32)
            cac[i0 : i0 + half, j0 : j0 + width] = jnp.where(keep > 0.5, cube, 0.0).astype(BF)
        if q == 0:
            relay(n_group + 1)
        done = mm(fm[...], cac[:, j0 : j0 + width])
        end = min(j0 + width, s_.cols)
        out_ref[:, j0:end] -= 0.5 * done[:, 0 : end - j0]

    for q in range(2):
        sent_share(n_group + q)


def on_device(hamiltonian, new_atom, pattern):
    rows, cols = hamiltonian.shape
    n_row, n_col = lax.axis_size("row"), lax.axis_size("col")
    ar, ac = pattern.shape
    s = Plan(n_row, n_col, rows, cols, ar, ac)
    vm = pl.BlockSpec(memory_space=pltpu.VMEM)
    dma = pltpu.SemaphoreType.DMA
    n_piece = len(s.sizes)
    n_group = len(s.groups)
    slots = n_col * s.slot
    buffers = [
        pltpu.VMEM((s.wide, s.blk), BF),
        pltpu.VMEM((n_row - 1, s.sl, s.blk), BF),
        pltpu.VMEM((n_row - 1, s.slp, s.blk), BF),
        pltpu.VMEM((s.av, LANE), F32),
        pltpu.VMEM((n_col, s.av, LANE), BF),
        pltpu.VMEM((s.live, s.w), BF),
        pltpu.VMEM((s.live, s.blk), BF),
        pltpu.VMEM((n_col, s.live, s.blk), BF),
        pltpu.VMEM((s.live, n_col * slots), BF),
        pltpu.VMEM((n_col, s.blk, LANE), F32),
        pltpu.VMEM((n_col * LANE, s.blk), BF),
        pltpu.VMEM((n_row, s.wide, s.blk), BF),
        pltpu.VMEM((n_col * slots, s.blk), BF),
        pltpu.VMEM((n_row, s.ratio * slots, s.wide) if s.stored else (n_row, 8, s.wide), BF if s.stored else F32),
        pltpu.VMEM((rows, s.wide), BF),
        pltpu.VMEM((n_row, s.wide, s.joff[0][1]), BF),
        pltpu.VMEM((n_row, s.wide, s.joff[1][1]), BF),
        pltpu.VMEM((s.wide, s.blk), BF),
        pltpu.VMEM((8, s.blk), F32),
        pltpu.VMEM((n_row, 8, LANE), F32),
    ]
    held = sum(int(np.prod(b.shape)) * np.dtype(b.dtype).itemsize for b in buffers)
    return pl.pallas_call(
        functools.partial(kernel, s, float(rows * n_row)),
        out_shape=jax.ShapeDtypeStruct((rows, cols), F32),
        in_specs=[vm, vm, vm],
        out_specs=vm,
        scratch_shapes=[
            *buffers,
            dma((n_row,)),
            dma((n_row,)),
            dma((n_col,)),
            dma((n_col,)),
            dma((n_row,)),
            dma((n_row,)),
            dma((3, n_col, n_piece)),
            dma((n_col, n_piece)),
            dma((n_group + 2, n_row)),
            dma((n_group + 2, n_row)),
            dma((n_group + 2, n_row)),
        ],
        compiler_params=pltpu.CompilerParams(
            collective_id=0, has_side_effects=True, vmem_limit_bytes=min(held + held // 8 + 7 * 1024 * 1024, 62 * 1024 * 1024)
        ),
    )(hamiltonian, new_atom.reshape(1, -1), pattern.T)


def solution(mesh):
    in_specs = (P("row", "col"), P(), P("row", "col"))
    out_specs = P("row", "col")
    return jax.shard_map(
        on_device, mesh=mesh, in_specs=in_specs, out_specs=out_specs, check_vma=False
    )
```
